32 devices in a mesh: member: 4 (over y, x), tile: 8 (over z, core).
Axes of the slice: x: 2, y: 2, z: 4, core: 2. Of those that a mesh axis runs over, the one named last changes fastest.
Arguments:
- northward_speed_field: float32 [16, 16, 64, 256], P('member', None, 'tile'), may hold values from -6 to 6
- level_depth_extent: float32 [16, 16, 64, 256], P('member', None, 'tile'), may hold values from 0.2 to 5
- potential_warmth_anomaly: float32 [16, 16, 64, 256], P('member', None, 'tile'), may hold values from -6 to 6
- ocean_region_label: int32 [64, 256], P('tile'), may hold values from 0 to 9
- zone_for_parallel: int32 [256], replicated, may hold values from 0 to 15, never falling along the last dimension, each value on 1 to 32 neighbouring positions
Outputs:
- mean_psi: float32 [10, 16, 256], P(None, None, ('member', 'tile'))
- mean_heat: float32 [10, 256], P(None, ('member', 'tile'))
- covariance: float32 [16, 16, 16], replicated
The draws below stay inside these ranges and needn't reach their ends.
Inputs may be any that keep to these rules, and one draw needn't show every extreme that they name: `zone_for_parallel`: never falls along latitude; every band holds 1 to 32 latitudes.
All inputs are finite; a program needn't handle non-finite values.
Results may differ from the reference program's by a relative error of at most 0.00011.
Values sent between devices are 32-bit elements; how exact they have to be, the bound alone decides.
No kernel may reach another device: no remote copies, remote signals or barrier semaphores. Data moves between devices by JAX's collectives and lax.ppermute only.
A program may use at most 128 MiB of HBM per device.

```python
import math
import jax
import jax.numpy as jnp
import numpy as np
from jax import lax

BASINS = 10
VERTICAL_LEVELS = 16
NBANDS = 16
RUN_REPLICAS = 16
EASTWARD_POINTS = 64
NORTHWARD_LINES = 256


def set_ends(array, stream_key, least, high):
    extent = array.shape
    spot = [jax.random.randint(jax.random.fold_in(stream_key, axis), (), 0, extent[axis]) for axis in range(len(extent))]
    array = array.at[tuple(spot)].set(least)
    longest = extent.index(max(extent))
    spot[longest] = (spot[longest] + 1) % extent[longest]
    return array.at[tuple(spot)].set(high)


def block_levels(rng, shape, pieces, least, high):
    gain = 1.0
    for dim, shards_of in pieces:
        draws = jax.random.uniform(jax.random.fold_in(jax.random.fold_in(rng, 6), dim), (shards_of,), jnp.float32, least / len(pieces), high / len(pieces))
        gain = gain * jnp.repeat(jnp.exp(draws), shape[dim] // shards_of).reshape((-1,) + (1,) * (len(shape) - 1 - dim))
    return gain


def profile(amount, total, most, slope):
    loads = [(1 << 20) // math.isqrt(grade ** slope) + 1 for grade in range(2, amount + 1)]
    spare, holding = total - most - (amount - 1), [1] * (amount - 1)
    while spare > 0:
        movable = [i for i in range(amount - 1) if holding[i] < most]
        mass, budget = sum([loads[i] for i in movable]), spare
        for i in movable:
            extra = min(most - holding[i], max(1, budget * loads[i] // mass), spare)
            holding[i] = holding[i] + extra
            spare = spare - extra
    return np.array([most] + holding)


def ragged_sizes(stream_key, count, total, bound, lean):
    if count == 2:
        one = jax.random.randint(stream_key, (), max(1, total - bound), min(bound, total - 1) + 1)
        return jnp.stack([one, total - one])
    sizes = jnp.asarray(profile(count, total, bound, lean), jnp.int32)
    couples = (count - 1) // 2
    giver, sink = sizes[1:1 + 2 * couples:2], sizes[2:2 + 2 * couples:2]
    margin = jnp.minimum(giver - 1, bound - sink)
    moved = jax.random.randint(jax.random.fold_in(stream_key, 1), (couples,), 0, 1 << 20) % (margin + 1)
    sizes = sizes.at[1:1 + 2 * couples:2].set(giver - moved).at[2:2 + 2 * couples:2].set(sink + moved)
    return sizes[jax.random.permutation(jax.random.fold_in(stream_key, 2), count)]


def centred(stream_key, extent, deviation, bound, cuts=(), kind=jnp.bfloat16):
    loudness = block_levels(stream_key, extent, cuts, -0.22, 0.18) if cuts else 1.0
    values = jax.random.normal(stream_key, extent, jnp.float32) * deviation * loudness
    return jnp.minimum(jnp.maximum(values, -bound), bound).astype(kind)


def setup_inputs(seed: int = 0) -> dict:
    arg_keys = jax.random.split(jax.random.key(seed), 6)
    northward_speed_field = centred(arg_keys[0], (RUN_REPLICAS, VERTICAL_LEVELS, EASTWARD_POINTS, NORTHWARD_LINES), 1.0, 6.0, ((0, 4), (2, 8)), jnp.float32)
    level_depth_extent = jnp.clip(jnp.exp(math.log(5.0) - 3.218876 * jax.random.uniform(arg_keys[1], (RUN_REPLICAS, VERTICAL_LEVELS, EASTWARD_POINTS, NORTHWARD_LINES), jnp.float32) ** block_levels(arg_keys[1], (RUN_REPLICAS, VERTICAL_LEVELS, EASTWARD_POINTS, NORTHWARD_LINES), ((0, 4), (2, 8)), -0.2, 0.2)), 0.2, 5.0)
    potential_warmth_anomaly = centred(arg_keys[2], (RUN_REPLICAS, VERTICAL_LEVELS, EASTWARD_POINTS, NORTHWARD_LINES), 1.0, 6.0, ((0, 4), (2, 8)), jnp.float32)
    ocean_region_label = set_ends(jax.random.randint(arg_keys[3], (EASTWARD_POINTS, NORTHWARD_LINES), 0, BASINS), jax.random.fold_in(arg_keys[3], 1), 0, BASINS - 1).astype(jnp.int32)
    zone_for_parallel = jnp.searchsorted(jnp.cumsum(ragged_sizes(arg_keys[4], NBANDS, NORTHWARD_LINES, NORTHWARD_LINES // 8, 1)), jnp.arange(NORTHWARD_LINES), side="right").astype(jnp.int32)
    return {"northward_speed_field": northward_speed_field, "level_depth_extent": level_depth_extent, "potential_warmth_anomaly": potential_warmth_anomaly, "ocean_region_label": ocean_region_label, "zone_for_parallel": zone_for_parallel}


def metric_factor(lats):
    index = jnp.arange(lats, dtype=jnp.float32)
    return jnp.cos((-80.0 + 160.0 * (index + 0.5) / lats) * (math.pi / 180.0))

def reference(northward_speed_field, level_depth_extent, potential_warmth_anomaly, ocean_region_label, zone_for_parallel):
    greatest_bound_value = lax.Precision.HIGHEST
    northward_volume_carriage = northward_speed_field * level_depth_extent * metric_factor(NORTHWARD_LINES)
    region_indicator_matrix = (ocean_region_label[None, :, :] == jnp.arange(BASINS, dtype=jnp.int32)[:, None, None]).astype(jnp.float32)
    transport = jnp.einsum('mkxl,bxl->mbkl', northward_volume_carriage, region_indicator_matrix, precision=greatest_bound_value) / math.sqrt(EASTWARD_POINTS)
    thermal_energy_integral = jnp.einsum('tzux,pux->tpx', northward_volume_carriage * potential_warmth_anomaly, region_indicator_matrix, precision=greatest_bound_value) / math.sqrt(EASTWARD_POINTS * VERTICAL_LEVELS)
    stream = jnp.cumsum(transport, axis=2)
    mean_psi = lax.optimization_barrier(jnp.mean(stream, axis=0))
    mean_heat = lax.optimization_barrier(jnp.mean(thermal_energy_integral, axis=0))
    anomaly = (stream - mean_psi).reshape(RUN_REPLICAS, BASINS * VERTICAL_LEVELS, NORTHWARD_LINES)
    products = jnp.einsum('mfl,nfl->lmn', anomaly, anomaly, precision=greatest_bound_value)
    band_hot = (zone_for_parallel[:, None] == jnp.arange(NBANDS, dtype=jnp.int32)[None, :]).astype(jnp.float32)
    norm = float((RUN_REPLICAS - 1) * BASINS * VERTICAL_LEVELS * (NORTHWARD_LINES // NBANDS))
    covariance = jnp.einsum('lmn,lc->cmn', products, band_hot, precision=greatest_bound_value) / norm
    return (mean_psi, mean_heat, covariance)
```

```python
import functools
import math

import jax
import jax.numpy as jnp
from jax import lax
from jax.experimental import pallas as pl
from jax.experimental.pallas import tpu as pltpu
from jax.sharding import PartitionSpec as P

BASINS = 10
NBANDS = 16
LANES = 128
SUB = 8
HEAT_LANES = 16
HIGHEST = lax.Precision.HIGHEST


def metric_factor(lats):
    index = jnp.arange(lats, dtype=jnp.float32)
    return jnp.cos((-80.0 + 160.0 * (index + 0.5) / lats) * (math.pi / 180.0))


def iota(shape, dim):
    return lax.broadcasted_iota(jnp.int32, shape, dim)


def log2(n):
    assert n & (n - 1) == 0
    return n.bit_length() - 1


def split_features(layers, members_here):
    feats = BASINS * layers
    rest = feats - LANES
    assert 0 < rest and rest * members_here == LANES and LANES % layers == 0
    return feats, rest


def partial_kernel(v_ref, h_ref, w_ref, region_ref, spacing_ref, keep_ref, send_ref, heat_ref,
                   *, members_here, layers, columns, groups, tiles):
    feats, rest = split_features(layers, members_here)
    core = lax.axis_index("tile") % 2
    lb = pl.program_id(0)
    halves = layers // SUB
    lshift = log2(layers)
    slots = members_here + 1
    pieces = LANES // SUB
    rows = iota((feats, 2 * LANES), 0)
    cols = iota((feats, 2 * LANES), 1)

    def running(m):
        feature = jnp.where(cols < LANES, cols, cols - m * rest)
        valid = (cols < LANES) | ((feature >= LANES) & (feature < feats))
        same = (rows >> lshift) == (feature >> lshift)
        return jnp.where(valid & same & (rows <= feature), 1.0, 0.0)

    hrows = iota((BASINS * SUB, LANES), 0)
    hcols = iota((BASINS * SUB, LANES), 1)
    heat_table = jnp.where((hrows >> log2(SUB)) == (hcols & (HEAT_LANES - 1)), 1.0, 0.0)
    heat_lane = iota((SUB, LANES), 1) >> log2(HEAT_LANES)

    def put(place, slot, even, odd):
        keep_ref[place, slot] = jnp.where(core == 0, even, odd)
        send_ref[place, slot] = jnp.where(core == 0, odd, even)

    @pl.when(lb == 0)
    def _():
        heat_ref[...] = jnp.zeros_like(heat_ref)

    dims = (((0,), (0,)), ((), ()))
    spacing = spacing_ref[...]
    region = [jnp.broadcast_to(region_ref[x : x + 1, :], (SUB, LANES)) for x in range(columns)]
    warm = [None] * columns
    extra = None
    packed = []
    for m in range(members_here):
        acc = [[None] * halves for _ in range(BASINS)]
        for x in range(columns):
            flux = []
            for k in range(halves):
                at = pl.ds(((m * layers) + k * SUB) * columns + x, SUB, stride=columns)
                one = v_ref[at, :] * h_ref[at, :] * spacing
                heat = one * w_ref[at, :]
                warm[x] = heat if warm[x] is None else warm[x] + heat
                flux.append(one)
            for b in range(BASINS):
                hit = region[x] == b
                for k in range(halves):
                    part = jnp.where(hit, flux[k], 0.0)
                    acc[b][k] = part if acc[b][k] is None else acc[b][k] + part
        stacked = jnp.concatenate([acc[b][k] for b in range(BASINS) for k in range(halves)], 0)
        stream = lax.dot_general(
            stacked, running(m), dims, precision=HIGHEST, preferred_element_type=jnp.float32
        )
        packed.append(stream[:, :LANES])
        extra = stream[:, LANES:] if extra is None else extra + stream[:, LANES:]
    packed.append(extra)
    basin_heat = []
    for b in range(BASINS):
        total = None
        for x in range(columns):
            part = jnp.where(region[x] == b, warm[x], 0.0)
            total = part if total is None else total + part
        basin_heat.append(total)
    heat = lax.dot_general(
        jnp.concatenate(basin_heat, 0), heat_table, dims,
        precision=HIGHEST, preferred_element_type=jnp.float32,
    )
    for row in range(0, pieces, 2):
        tile = row % tiles
        group = lb * (pieces // tiles) + row // tiles
        even = slice(row * SUB, (row + 1) * SUB)
        odd = slice((row + 1) * SUB, (row + 2) * SUB)
        for s in range(slots):
            put(tile // 2, group * slots + s, packed[s][even], packed[s][odd])
        heat_ref[tile] += jnp.where(heat_lane == group, heat[even], 0.0)
        heat_ref[tile + 1] += jnp.where(heat_lane == group, heat[odd], 0.0)

    @pl.when(lb == pl.num_programs(0) - 1)
    def _():
        for tile in range(0, tiles, 2):
            put(tile // 2, groups * slots, heat_ref[tile], heat_ref[tile + 1])


def gather_kernel(*refs, members_here, layers, groups, tiles):
    zone_ref = refs[0]
    parts = refs[1 : 1 + groups]
    psi_ref, heat_ref, cov_ref, all_ref, mean_ref = refs[1 + groups :]
    feats, rest = split_features(layers, members_here)
    slots = members_here + 1
    members = members_here * groups
    mine = lax.axis_index("member")
    tile = lax.axis_index("tile")
    for r in range(groups):
        all_ref[mine ^ r] = parts[r][...]
    wide = members * SUB
    lane = iota((SUB, LANES), 1)
    sshift, jmask = log2(SUB), SUB - 1
    same_lat = (iota((wide, wide), 0) & jmask) == (iota((wide, wide), 1) & jmask)
    pick = jnp.where(iota((members, wide), 0) == (iota((members, wide), 1) >> sshift), 1.0, 0.0)
    qrow = iota((NBANDS * members, wide), 0)
    qcol = iota((NBANDS * members, wide), 1)
    same_member = (qrow & (members - 1)) == (qcol >> sshift)
    qband = qrow >> log2(members)
    lat_lane = iota((1, wide), 1) & jmask
    last = (((1,), (1,)), ((), ()))
    dot = functools.partial(
        lax.dot_general, precision=HIGHEST, preferred_element_type=jnp.float32
    )
    total = None
    for g in range(groups):
        heads, tails = [], []
        for q in range(groups):
            tail = all_ref[q, g * slots + members_here]
            for m in range(members_here):
                heads.append(all_ref[q, g * slots + m])
                moved = tail if m == 0 else pltpu.roll(tail, LANES - m * rest, 1)
                tails.append(jnp.where(lane < rest, moved, 0.0))
        head_mean = sum(heads) * (1.0 / members)
        tail_mean = sum(tails) * (1.0 / members)
        mean_ref[g, 0] = head_mean
        mean_ref[g, 1] = tail_mean
        head = jnp.concatenate([a - head_mean for a in heads], 0)
        tail = jnp.concatenate([a - tail_mean for a in tails], 0)
        gram = dot(head, head, last) + dot(tail, tail, last)
        gram = jnp.where(same_lat, gram, 0.0)
        summed = dot(pick, gram, (((1,), (0,)), ((), ())))
        zone = jnp.zeros((1, wide), jnp.int32)
        for j in range(SUB):
            zone = jnp.where(lat_lane == j, zone_ref[(g * tiles + tile) * SUB + j], zone)
        chosen = jnp.where(same_member & (qband == zone), 1.0, 0.0)
        share = dot(summed, chosen, last)
        total = share if total is None else total + share
    cov_ref[...] = total
    for b in range(BASINS):
        half, at = divmod(b * layers, LANES)
        psi_ref[b] = mean_ref[mine, half][:, at : at + layers]
    warm = sum(all_ref[q, groups * slots] for q in range(groups))
    out = jnp.zeros((SUB, BASINS), jnp.float32)
    for g in range(groups):
        out = jnp.where(mine == g, warm[:, g * HEAT_LANES : g * HEAT_LANES + BASINS], out)
    heat_ref[...] = out * (1.0 / (members * math.sqrt(layers)))


def unpack_kernel(*refs, members, scale):
    out_ref = refs[-1]
    total = refs[0][...]
    for ref in refs[1:-1]:
        total = total + ref[...]
    total = total * scale
    for c in range(NBANDS):
        out_ref[c] = total[:, c * members : (c + 1) * members]


def exchange(value, axis, bit):
    size = lax.axis_size(axis)
    return lax.ppermute(value, axis, [(i, i ^ bit) for i in range(size)])


VMEM = pl.BlockSpec(memory_space=pltpu.MemorySpace.VMEM)
SMEM = pl.BlockSpec(memory_space=pltpu.MemorySpace.SMEM)


def local(
    northward_speed_field,
    level_depth_extent,
    potential_warmth_anomaly,
    ocean_region_label,
    zone_for_parallel,
):
    members_here, layers, columns, lats = northward_speed_field.shape
    tiles = lax.axis_size("tile")
    groups = lax.axis_size("member")
    members = members_here * groups
    slots = groups * (members_here + 1) + 1
    assert lats == groups * tiles * SUB and (LANES // SUB) % tiles == 0 and groups * HEAT_LANES <= LANES
    spacing = (metric_factor(lats) / math.sqrt(columns * tiles)).reshape(1, lats)
    flat = (members_here * layers * columns, lats)
    piece = jax.ShapeDtypeStruct((tiles // 2, slots, SUB, LANES), jnp.float32)
    keep, send = pl.pallas_call(
        functools.partial(
            partial_kernel, members_here=members_here, layers=layers, columns=columns,
            groups=groups, tiles=tiles,
        ),
        out_shape=(piece, piece),
        grid=(lats // LANES,),
        in_specs=[
            pl.BlockSpec((flat[0], LANES), lambda i: (0, i)),
            pl.BlockSpec((flat[0], LANES), lambda i: (0, i)),
            pl.BlockSpec((flat[0], LANES), lambda i: (0, i)),
            pl.BlockSpec((columns, LANES), lambda i: (0, i)),
            pl.BlockSpec((1, LANES), lambda i: (0, i)),
        ],
        out_specs=(
            pl.BlockSpec(piece.shape, lambda i: (0, 0, 0, 0)),
            pl.BlockSpec(piece.shape, lambda i: (0, 0, 0, 0)),
        ),
        scratch_shapes=[pltpu.VMEM((tiles, SUB, LANES), jnp.float32)],
        name="partial",
    )(
        northward_speed_field.reshape(flat),
        level_depth_extent.reshape(flat),
        potential_warmth_anomaly.reshape(flat),
        ocean_region_label,
        spacing,
    )
    tile = lax.axis_index("tile")
    got = exchange(send, "tile", 1)
    bit = 2
    while bit < tiles:
        shape = (keep.shape[0] // 2, 2) + keep.shape[1:]
        keep, got = keep.reshape(shape), got.reshape(shape)
        mine = (tile // bit) % 2
        send = lax.dynamic_index_in_dim(keep, 1 - mine, 1, False) + lax.dynamic_index_in_dim(
            got, 1 - mine, 1, False
        )
        keep = lax.dynamic_index_in_dim(keep, mine, 1, False) + lax.dynamic_index_in_dim(
            got, mine, 1, False
        )
        got = exchange(send, "tile", bit)
        bit *= 2
    owned = (keep + got).reshape(slots, SUB, LANES)
    parts = [owned] + [exchange(owned, "member", r) for r in range(1, groups)]
    psi, heat, share = pl.pallas_call(
        functools.partial(
            gather_kernel, members_here=members_here, layers=layers, groups=groups, tiles=tiles
        ),
        out_shape=(
            jax.ShapeDtypeStruct((BASINS, SUB, layers), jnp.float32),
            jax.ShapeDtypeStruct((SUB, BASINS), jnp.float32),
            jax.ShapeDtypeStruct((members, NBANDS * members), jnp.float32),
        ),
        in_specs=[SMEM] + [VMEM] * groups,
        out_specs=(VMEM, VMEM, VMEM),
        scratch_shapes=[
            pltpu.VMEM((groups, slots, SUB, LANES), jnp.float32),
            pltpu.VMEM((groups, 2, SUB, LANES), jnp.float32),
        ],
        name="gather",
    )(zone_for_parallel, *parts)
    bit = 1
    while 2 * bit < tiles:
        share = share + exchange(share, "tile", bit)
        bit *= 2
    norm = float((members - 1) * BASINS * layers * (lats // NBANDS))
    covariance = pl.pallas_call(
        functools.partial(unpack_kernel, members=members, scale=1.0 / norm),
        out_shape=jax.ShapeDtypeStruct((NBANDS, members, members), jnp.float32),
        in_specs=[VMEM] * 2,
        out_specs=VMEM,
        name="unpack",
    )(share, exchange(share, "tile", bit))
    return (jnp.transpose(psi, (0, 2, 1)), jnp.transpose(heat, (1, 0)), covariance)


def solution(mesh):
    in_specs = (
        P("member", None, "tile", None),
        P("member", None, "tile", None),
        P("member", None, "tile", None),
        P("tile", None),
        P(),
    )
    out_specs = (P(None, None, ("member", "tile")), P(None, ("member", "tile")), P())
    return jax.shard_map(local, mesh=mesh, in_specs=in_specs, out_specs=out_specs, check_vma=False)
```

```python
import functools
import math

import jax
import jax.numpy as jnp
from jax import lax
from jax.experimental import pallas as pl
from jax.experimental.pallas import tpu as pltpu
from jax.sharding import PartitionSpec as P

BASINS = 10
NBANDS = 16
LANES = 128
SUB = 8
HEAT_LANES = 16
HIGHEST = lax.Precision.HIGHEST


def metric_factor(lats):
    index = jnp.arange(lats, dtype=jnp.float32)
    return jnp.cos((-80.0 + 160.0 * (index + 0.5) / lats) * (math.pi / 180.0))


def iota(shape, dim):
    return lax.broadcasted_iota(jnp.int32, shape, dim)


def log2(n):
    assert n & (n - 1) == 0
    return n.bit_length() - 1


def split_features(layers, members_here):
    feats = BASINS * layers
    rest = feats - LANES
    assert 0 < rest and rest * members_here == LANES and LANES % layers == 0
    return feats, rest


def exact_parts(x):
    parts = []
    for _ in range(3):
        parts.append(x.astype(jnp.bfloat16))
        x = x - parts[-1].astype(jnp.float32)
    return parts


def partial_kernel(v_ref, h_ref, w_ref, region_ref, spacing_ref, keep0_ref, send0_ref,
                   keep1_ref, send1_ref, buf, small, sems, small_sem,
                   *, half, members_here, layers, columns, groups, tiles):
    feats, rest = split_features(layers, members_here)
    core = lax.axis_index("tile") % 2
    halves = layers // SUB
    lshift = log2(layers)
    slots = members_here + 1
    pieces = LANES // SUB
    blocks = 2 * half
    inputs = (v_ref, h_ref, w_ref)
    per = layers * blocks * columns

    def fetch(m, a):
        part = pl.ds(m * per, per)
        return pltpu.make_async_copy(inputs[a].at[part], buf.at[a, part], sems.at[m, a])

    labels = pltpu.make_async_copy(region_ref, small, small_sem)
    labels.start()
    for m in range(members_here):
        for a in range(3):
            fetch(m, a).start()
    rows = iota((feats, feats), 0)
    cols = iota((feats, feats), 1)
    running = ((rows >> lshift) == (cols >> lshift)) & (cols <= rows)
    running = jnp.where(running, 1.0, 0.0).astype(jnp.bfloat16)
    rows = iota((LANES, BASINS * SUB), 0)
    cols = iota((LANES, BASINS * SUB), 1)
    gather = jnp.where((rows & (HEAT_LANES - 1)) == (cols >> log2(SUB)), 1.0, 0.0)
    gather = gather.astype(jnp.bfloat16)
    heat_group = iota((LANES, LANES), 0) >> log2(HEAT_LANES)
    heat_lat = iota((LANES, LANES), 1)

    def select(table, x):
        return jnp.dot(
            jnp.concatenate([table] * 3, 1), jnp.concatenate(exact_parts(x), 0),
            preferred_element_type=jnp.float32,
        )

    def put(late, place, slot, even, odd):
        keep_ref, send_ref = (keep1_ref, send1_ref) if late else (keep0_ref, send0_ref)
        keep_ref[place, slot] = jnp.where(core == 0, even, odd)
        send_ref[place, slot] = jnp.where(core == 0, odd, even)

    def put_block(lb, s, value):
        for row in range(0, pieces, 2):
            group, tile = divmod(lb * pieces + row, tiles)
            late = group >= groups // 2
            slot = (group - late * (groups // 2)) * slots + s
            even = value[row * SUB : (row + 1) * SUB]
            put(late, tile // 2, slot, even, value[(row + 1) * SUB : (row + 2) * SUB])

    warm = [[None] * columns for _ in range(blocks)]
    extra = [[] for _ in range(blocks)]
    labels.wait()
    region, spacing = small[...], spacing_ref[...]

    def label(lb, x):
        line = region[x : x + 1, lb * LANES : (lb + 1) * LANES]
        return jnp.broadcast_to(line, (SUB, LANES))

    for m in range(members_here):
        for a in range(3):
            fetch(m, a).wait()
        for lb in range(blocks):
            scale = spacing[:, lb * LANES : (lb + 1) * LANES]
            acc = [[None] * halves for _ in range(BASINS)]
            for x in range(columns):
                flux = []
                for k in range(halves):
                    start = m * per + (k * SUB * blocks + lb) * columns + x
                    at = pl.ds(start, SUB, stride=blocks * columns)
                    one = buf[0, at, :] * buf[1, at, :] * scale
                    heat = one * buf[2, at, :]
                    warm[lb][x] = heat if warm[lb][x] is None else warm[lb][x] + heat
                    flux.append(one)
                here = label(lb, x)
                for b in range(BASINS):
                    hit = here == b
                    for k in range(halves):
                        part = jnp.where(hit, flux[k], 0.0)
                        acc[b][k] = part if acc[b][k] is None else acc[b][k] + part
            stacked = jnp.concatenate([acc[b][k] for b in range(BASINS) for k in range(halves)], 0)
            stream = select(running, stacked)
            put_block(lb, m, stream[:LANES].T)
            extra[lb].append(stream[LANES:])
    span = tiles * SUB
    heat = None
    for lb in range(blocks):
        put_block(lb, members_here, jnp.concatenate(extra[lb], 0).T)
        basin_heat = []
        for b in range(BASINS):
            total = None
            for x in range(columns):
                part = jnp.where(label(lb, x) == b, warm[lb][x], 0.0)
                total = part if total is None else total + part
            basin_heat.append(total)
        block = select(gather, jnp.concatenate(basin_heat, 0))
        for p in range(LANES // span):
            moved = block if p == 0 else pltpu.roll(block, LANES - p * span, 1)
            mine = (heat_group == lb * (LANES // span) + p) & (heat_lat < span)
            part = jnp.where(mine, moved, 0.0)
            heat = part if heat is None else heat + part
    heat = heat.T
    for t in range(0, tiles, 2):
        even = heat[t * SUB : (t + 1) * SUB]
        put(True, t // 2, slots * (groups // 2), even, heat[(t + 1) * SUB : (t + 2) * SUB])


def bands_kernel(zone_ref, order_ref, out_ref, *, members, groups, tiles):
    tile = lax.axis_index("tile")
    wide = members * SUB
    sshift = log2(SUB)
    row = iota((NBANDS * members, wide), 0)
    col = iota((NBANDS * members, wide), 1)
    same_member = (row & (members - 1)) == (col >> sshift)
    band = row >> log2(members)
    lat_lane = iota((1, wide), 1) & (SUB - 1)
    for g in range(groups):
        zone = jnp.zeros((1, wide), jnp.int32)
        for j in range(SUB):
            zone = jnp.where(lat_lane == j, zone_ref[(g * tiles + tile) * SUB + j], zone)
        hit = jnp.where(same_member & (band == zone), 1.0, 0.0)
        out_ref[g] = hit.astype(jnp.bfloat16)


def share_kernel(*refs, members_here, layers, groups):
    bands_ref = refs[0]
    parts = refs[1 : 1 + groups]
    cov_ref, all_ref = refs[1 + groups :]
    feats, rest = split_features(layers, members_here)
    slots = members_here + 1
    members = members_here * groups
    mine = lax.axis_index("member")
    for r in range(groups):
        all_ref[mine ^ r] = parts[r][: groups * slots]
    wide = members * SUB
    lane = iota((SUB, LANES), 1)
    jmask = SUB - 1
    same_lat = (iota((SUB, wide), 0)) == (iota((SUB, wide), 1) & jmask)
    last = (((1,), (1,)), ((), ()))
    total = None
    for g in range(groups):
        heads, tails = [], []
        for q in range(groups):
            tail = all_ref[q, g * slots + members_here]
            for m in range(members_here):
                heads.append(all_ref[q, g * slots + m])
                moved = tail if m == 0 else pltpu.roll(tail, LANES - m * rest, 1)
                tails.append(jnp.where(lane < rest, moved, 0.0))
        head_mean = sum(heads) * (1.0 / members)
        tail_mean = sum(tails) * (1.0 / members)
        head = jnp.concatenate([a - head_mean for a in heads], 0)
        tail = jnp.concatenate([a - tail_mean for a in tails], 0)
        both = jnp.concatenate([head, tail], 1)
        gram = lax.dot_general(
            both, both, last, precision=HIGHEST, preferred_element_type=jnp.float32
        )
        summed = jnp.concatenate(
            [
                jnp.sum(
                    jnp.where(same_lat, gram[n * SUB : (n + 1) * SUB], 0.0), axis=0, keepdims=True
                )
                for n in range(members)
            ],
            0,
        )
        share = lax.dot_general(
            jnp.concatenate(exact_parts(summed), 0), bands_ref[g], last,
            preferred_element_type=jnp.float32,
        )
        total = share if total is None else total + share
    cov_ref[...] = total[:members] + (total[members : 2 * members] + total[2 * members :])


def means_kernel(*refs, members_here, layers, groups):
    parts = refs[:groups]
    psi_ref, heat_ref = refs[groups:]
    feats, rest = split_features(layers, members_here)
    slots = members_here + 1
    members = members_here * groups
    mine = lax.axis_index("member")
    at = mine * slots

    def total(slot):
        return sum(ref[slot] for ref in parts)

    head = sum(total(at + m) for m in range(members_here)) * (1.0 / members)
    packed = total(at + members_here)
    tail = packed
    for m in range(1, members_here):
        tail = tail + pltpu.roll(packed, LANES - m * rest, 1)
    tail = tail * (1.0 / members)
    for b in range(BASINS):
        part, lane = divmod(b * layers, LANES)
        psi_ref[b] = (tail if part else head)[:, lane : lane + layers]
    warm = total(groups * slots)
    out = jnp.zeros((SUB, BASINS), jnp.float32)
    for g in range(groups):
        out = jnp.where(mine == g, warm[:, g * HEAT_LANES : g * HEAT_LANES + BASINS], out)
    heat_ref[...] = out * (1.0 / (members * math.sqrt(layers)))


def unpack_kernel(*refs, members, scale):
    out_ref = refs[-1]
    total = refs[0][...]
    for ref in refs[1:-1]:
        total = total + ref[...]
    total = total * scale
    for c in range(NBANDS):
        out_ref[c] = total[:, c * members : (c + 1) * members]


def exchange(value, axis, bit):
    size = lax.axis_size(axis)
    return lax.ppermute(value, axis, [(i, i ^ bit) for i in range(size)])


def halve(keep, got, tile, bit):
    shape = (keep.shape[0] // 2, 2) + keep.shape[1:]
    keep, got = keep.reshape(shape), got.reshape(shape)
    mine = (tile // bit) % 2
    send, keep = (
        lax.dynamic_index_in_dim(keep, side, 1, False)
        + lax.dynamic_index_in_dim(got, side, 1, False)
        for side in (1 - mine, mine)
    )
    return keep, exchange(send, "tile", bit)


ANY = pl.BlockSpec(memory_space=pl.ANY)
VMEM = pl.BlockSpec(memory_space=pltpu.MemorySpace.VMEM)
PARAMS = pltpu.CompilerParams(vmem_limit_bytes=16 * 1024 * 1024)
SMEM = pl.BlockSpec(memory_space=pltpu.MemorySpace.SMEM)


def local(
    northward_speed_field,
    level_depth_extent,
    potential_warmth_anomaly,
    ocean_region_label,
    zone_for_parallel,
):
    members_here, layers, columns, lats = northward_speed_field.shape
    tiles = lax.axis_size("tile")
    groups = lax.axis_size("member")
    members = members_here * groups
    per_block = LANES // SUB // tiles
    half = lats // LANES // 2
    count = groups // 2
    slots = members_here + 1
    assert lats == groups * tiles * SUB and groups * HEAT_LANES <= LANES
    assert half >= 1 and half * per_block == count and lats == 2 * half * LANES
    spacing = (metric_factor(lats) / math.sqrt(columns * tiles)).reshape(1, lats)
    rows = members_here * layers * columns
    sizes = dict(
        half=half, members_here=members_here, layers=layers, columns=columns,
        groups=groups, tiles=tiles,
    )
    inputs = (northward_speed_field, level_depth_extent, potential_warmth_anomaly)
    blocked = [
        pltpu.with_memory_space_constraint(
            x.reshape(rows // columns, columns, 2 * half, LANES)
            .transpose(0, 2, 1, 3)
            .reshape(2 * half * rows, LANES),
            pltpu.MemorySpace.HBM,
        )
        for x in (northward_speed_field, level_depth_extent, potential_warmth_anomaly)
    ]
    labels = pltpu.with_memory_space_constraint(ocean_region_label, pltpu.MemorySpace.HBM)
    early = pltpu.VMEM((tiles // 2, count * slots, SUB, LANES), jnp.float32)
    late = pltpu.VMEM((tiles // 2, count * slots + 1, SUB, LANES), jnp.float32)
    keep0, send0, keep1, send1 = pl.pallas_call(
        functools.partial(partial_kernel, **sizes),
        out_shape=(early, early, late, late),
        in_specs=[ANY] * 4 + [VMEM],
        out_specs=(VMEM,) * 4,
        scratch_shapes=[
            pltpu.VMEM((3, 2 * half * rows, LANES), jnp.float32),
            pltpu.VMEM((columns, lats), jnp.int32),
            pltpu.SemaphoreType.DMA((members_here, 3)),
            pltpu.SemaphoreType.DMA(()),
        ],
        compiler_params=PARAMS,
        name="partial",
    )(*blocked, labels, spacing)
    got0 = exchange(send0, "tile", 1)
    got1 = exchange(send1, "tile", 1)
    bands = pl.pallas_call(
        functools.partial(bands_kernel, members=members, groups=groups, tiles=tiles),
        out_shape=pltpu.VMEM((groups, NBANDS * members, members * SUB), jnp.bfloat16),
        in_specs=[SMEM, ANY],
        out_specs=VMEM,
        compiler_params=PARAMS,
        name="bands",
    )(zone_for_parallel, got0)
    tile = lax.axis_index("tile")
    chunks = [(keep0, got0), (keep1, got1)]
    bit = 2
    while bit < tiles:
        chunks = [halve(keep, got, tile, bit) for keep, got in chunks]
        bit *= 2
    owned = jnp.concatenate([(keep + got)[0] for keep, got in chunks], 0)
    parts = [owned] + [exchange(owned, "member", r) for r in range(1, groups)]
    known = dict(members_here=members_here, layers=layers, groups=groups)
    share = pl.pallas_call(
        functools.partial(share_kernel, **known),
        out_shape=pltpu.VMEM((members, NBANDS * members), jnp.float32),
        in_specs=[VMEM] * (1 + groups),
        out_specs=VMEM,
        scratch_shapes=[pltpu.VMEM((groups, groups * slots, SUB, LANES), jnp.float32)],
        compiler_params=PARAMS,
        name="share",
    )(bands, *parts)
    psi, heat = pl.pallas_call(
        functools.partial(means_kernel, **known),
        out_shape=(
            jax.ShapeDtypeStruct((BASINS, SUB, layers), jnp.float32),
            jax.ShapeDtypeStruct((SUB, BASINS), jnp.float32),
        ),
        in_specs=[VMEM] * groups,
        out_specs=(VMEM, VMEM),
        compiler_params=PARAMS,
        name="means",
    )(*parts)
    bit = 1
    while 2 * bit < tiles:
        share = share + exchange(share, "tile", bit)
        bit *= 2
    norm = float((members - 1) * BASINS * layers * (lats // NBANDS))
    covariance = pl.pallas_call(
        functools.partial(unpack_kernel, members=members, scale=1.0 / norm),
        out_shape=jax.ShapeDtypeStruct((NBANDS, members, members), jnp.float32),
        in_specs=[VMEM] * 2,
        out_specs=VMEM,
        compiler_params=PARAMS,
        name="unpack",
    )(share, exchange(share, "tile", bit))
    return (jnp.transpose(psi, (0, 2, 1)), jnp.transpose(heat, (1, 0)), covariance)


def solution(mesh):
    in_specs = (
        P("member", None, "tile", None),
        P("member", None, "tile", None),
        P("member", None, "tile", None),
        P("tile", None),
        P(),
    )
    out_specs = (P(None, None, ("member", "tile")), P(None, ("member", "tile")), P())
    return jax.shard_map(local, mesh=mesh, in_specs=in_specs, out_specs=out_specs, check_vma=False)
```

```python
import functools
import math

import jax
import jax.numpy as jnp
from jax import lax
from jax.experimental import pallas as pl
from jax.experimental.pallas import tpu as pltpu
from jax.sharding import PartitionSpec as P


BASINS = 10
NBANDS = 16
LANES = 128
SUB = 8
HEAT_LANES = 16


def metric_factor(lats):
    index = jnp.arange(lats, dtype=jnp.float32)
    return jnp.cos((-80.0 + 160.0 * (index + 0.5) / lats) * (math.pi / 180.0))


def iota(shape, dim):
    return lax.broadcasted_iota(jnp.int32, shape, dim)


def log2(n):
    assert n & (n - 1) == 0
    return n.bit_length() - 1


def split_features(layers, members_here):
    feats = BASINS * layers
    rest = feats - LANES
    assert 0 < rest and rest * members_here == LANES and LANES % layers == 0
    return feats, rest


def exact_parts(x):
    parts = []
    for _ in range(3):
        parts.append(x.astype(jnp.bfloat16))
        x = x - parts[-1].astype(jnp.float32)
    return parts


def basin_sums(buf, region, spacing, heat_ref, keep_ref, send_ref,
               *, late, half, members_here, layers, columns, groups, tiles):
    feats, _ = split_features(layers, members_here)
    core = lax.axis_index("tile") % 2
    halves = layers // SUB
    lshift = log2(layers)
    slots = members_here + 1
    pieces = LANES // SUB
    blocks = 2 * half
    per = layers * blocks * columns
    mine = range(half, blocks) if late else range(half)
    rows = iota((feats, feats), 0)
    cols = iota((feats, feats), 1)
    running = ((rows >> lshift) == (cols >> lshift)) & (cols <= rows)
    running = jnp.where(running, 1.0, 0.0).astype(jnp.bfloat16)
    rows = iota((LANES, BASINS * SUB), 0)
    cols = iota((LANES, BASINS * SUB), 1)
    gather = jnp.where((rows & (HEAT_LANES - 1)) == (cols >> log2(SUB)), 1.0, 0.0)
    gather = gather.astype(jnp.bfloat16)
    heat_group = iota((LANES, LANES), 0) >> log2(HEAT_LANES)
    heat_lat = iota((LANES, LANES), 1)

    def select(table, x):
        return jnp.dot(
            jnp.concatenate([table] * 3, 1), jnp.concatenate(exact_parts(x), 0),
            preferred_element_type=jnp.float32,
        )

    def put(place, slot, even, odd):
        keep_ref[place, slot] = jnp.where(core == 0, even, odd)
        send_ref[place, slot] = jnp.where(core == 0, odd, even)

    def put_block(lb, s, value):
        for row in range(0, pieces, 2):
            group, tile = divmod(lb * pieces + row, tiles)
            slot = (group % (groups // 2)) * slots + s
            even = value[row * SUB : (row + 1) * SUB]
            put(tile // 2, slot, even, value[(row + 1) * SUB : (row + 2) * SUB])

    warm = [[None] * columns for _ in range(blocks)]
    extra = [[] for _ in range(blocks)]

    def label(lb, x):
        line = region[x : x + 1, lb * LANES : (lb + 1) * LANES]
        return jnp.broadcast_to(line, (SUB, LANES))

    for m in range(members_here):
        for lb in mine:
            scale = spacing[:, lb * LANES : (lb + 1) * LANES]
            acc = [[None] * halves for _ in range(BASINS)]
            for x in range(columns):
                flux = []
                for k in range(halves):
                    start = m * per + (k * SUB * blocks + lb) * columns + x
                    at = pl.ds(start, SUB, stride=blocks * columns)
                    one = buf[0, at, :] * buf[1, at, :] * scale
                    heat = one * buf[2, at, :]
                    warm[lb][x] = heat if warm[lb][x] is None else warm[lb][x] + heat
                    flux.append(one)
                here = label(lb, x)
                for b in range(BASINS):
                    hit = here == b
                    for k in range(halves):
                        part = jnp.where(hit, flux[k], 0.0)
                        acc[b][k] = part if acc[b][k] is None else acc[b][k] + part
            stacked = jnp.concatenate([acc[b][k] for b in range(BASINS) for k in range(halves)], 0)
            stream = select(running, stacked)
            put_block(lb, m, stream[:LANES].T)
            extra[lb].append(stream[LANES:])
    span = tiles * SUB
    heat = heat_ref[...] if late else None
    for lb in mine:
        put_block(lb, members_here, jnp.concatenate(extra[lb], 0).T)
        basin_heat = []
        for b in range(BASINS):
            total = None
            for x in range(columns):
                part = jnp.where(label(lb, x) == b, warm[lb][x], 0.0)
                total = part if total is None else total + part
            basin_heat.append(total)
        block = select(gather, jnp.concatenate(basin_heat, 0))
        for p in range(LANES // span):
            moved = block if p == 0 else pltpu.roll(block, LANES - p * span, 1)
            keep = (heat_group == lb * (LANES // span) + p) & (heat_lat < span)
            part = jnp.where(keep, moved, 0.0)
            heat = part if heat is None else heat + part
    if not late:
        heat_ref[...] = heat
        return
    heat = heat.T
    for t in range(0, tiles, 2):
        even = heat[t * SUB : (t + 1) * SUB]
        put(t // 2, slots * (groups // 2), even, heat[(t + 1) * SUB : (t + 2) * SUB])


def first_kernel(v_ref, h_ref, w_ref, region_ref, spacing_ref, keep_ref, send_ref, heat_ref,
                 data_ref, small_ref, sems, small_sem, **sizes):
    copies = [pltpu.make_async_copy(region_ref, small_ref, small_sem)]
    for a, ref in enumerate((v_ref, h_ref, w_ref)):
        copies.append(pltpu.make_async_copy(ref, data_ref.at[a], sems.at[a]))
    for copy in copies:
        copy.start(priority=1)
    for copy in copies:
        copy.wait()
    basin_sums(
        data_ref, small_ref[...], spacing_ref[...], heat_ref, keep_ref, send_ref,
        late=False, **sizes,
    )


def second_kernel(data_ref, region_ref, spacing_ref, heat_ref, keep_ref, send_ref, **sizes):
    basin_sums(
        data_ref, region_ref[...], spacing_ref[...], heat_ref, keep_ref, send_ref,
        late=True, **sizes,
    )


def bands_kernel(zone_ref, order_ref, out_ref, *, members, groups, tiles):
    tile = lax.axis_index("tile")
    wide = members * SUB
    sshift = log2(SUB)
    row = iota((NBANDS * members, wide), 0)
    col = iota((NBANDS * members, wide), 1)
    same_member = (row & (members - 1)) == (col >> sshift)
    band = row >> log2(members)
    lat_lane = iota((1, wide), 1) & (SUB - 1)
    for g in range(groups):
        zone = jnp.zeros((1, wide), jnp.int32)
        for j in range(SUB):
            zone = jnp.where(lat_lane == j, zone_ref[(g * tiles + tile) * SUB + j], zone)
        hit = jnp.where(same_member & (band == zone), 1.0, 0.0)
        out_ref[g] = hit.astype(jnp.bfloat16)


def share_kernel(*refs, members_here, layers, groups):
    bands_ref = refs[0]
    parts = refs[1 : 1 + groups]
    cov_ref, all_ref = refs[1 + groups :]
    _, rest = split_features(layers, members_here)
    slots = members_here + 1
    members = members_here * groups
    mine = lax.axis_index("member")
    for r in range(groups):
        all_ref[mine ^ r] = parts[r][: groups * slots]
    wide = members * SUB
    lane = iota((SUB, LANES), 1)
    jmask = SUB - 1
    same_lat = (iota((SUB, wide), 0)) == (iota((SUB, wide), 1) & jmask)
    last = (((1,), (1,)), ((), ()))
    total = None
    for g in range(groups):
        heads, tails = [], []
        for q in range(groups):
            tail = all_ref[q, g * slots + members_here]
            for m in range(members_here):
                heads.append(all_ref[q, g * slots + m])
                moved = tail if m == 0 else pltpu.roll(tail, LANES - m * rest, 1)
                tails.append(jnp.where(lane < rest, moved, 0.0))
        head_mean = sum(heads) * (1.0 / members)
        tail_mean = sum(tails) * (1.0 / members)
        head = jnp.concatenate([a - head_mean for a in heads], 0)
        tail = jnp.concatenate([a - tail_mean for a in tails], 0)
        both = jnp.concatenate([head, tail], 1)
        high = both.astype(jnp.bfloat16)
        low = (both - high.astype(jnp.float32)).astype(jnp.bfloat16)
        gram = lax.dot_general(
            jnp.concatenate([high, high, low], 1), jnp.concatenate([high, low, high], 1),
            last, preferred_element_type=jnp.float32,
        )
        summed = jnp.concatenate(
            [
                jnp.sum(
                    jnp.where(same_lat, gram[n * SUB : (n + 1) * SUB], 0.0), axis=0, keepdims=True
                )
                for n in range(members)
            ],
            0,
        )
        share = lax.dot_general(
            jnp.concatenate(exact_parts(summed), 0), bands_ref[g], last,
            preferred_element_type=jnp.float32,
        )
        total = share if total is None else total + share
    cov_ref[...] = total[:members] + (total[members : 2 * members] + total[2 * members :])


def means_kernel(*refs, members_here, layers, groups):
    parts = refs[:groups]
    psi_ref, heat_ref = refs[groups:]
    _, rest = split_features(layers, members_here)
    slots = members_here + 1
    members = members_here * groups
    mine = lax.axis_index("member")
    at = mine * slots

    def total(slot):
        return sum(ref[slot] for ref in parts)

    head = sum(total(at + m) for m in range(members_here)) * (1.0 / members)
    packed = total(at + members_here)
    tail = packed
    for m in range(1, members_here):
        tail = tail + pltpu.roll(packed, LANES - m * rest, 1)
    tail = tail * (1.0 / members)
    for b in range(BASINS):
        part, lane = divmod(b * layers, LANES)
        psi_ref[b] = (tail if part else head)[:, lane : lane + layers]
    warm = total(groups * slots)
    out = jnp.zeros((SUB, BASINS), jnp.float32)
    for g in range(groups):
        out = jnp.where(mine == g, warm[:, g * HEAT_LANES : g * HEAT_LANES + BASINS], out)
    heat_ref[...] = out * (1.0 / (members * math.sqrt(layers)))


def unpack_kernel(*refs, members, scale):
    out_ref = refs[-1]
    total = refs[0][...]
    for ref in refs[1:-1]:
        total = total + ref[...]
    total = total * scale
    for c in range(NBANDS):
        out_ref[c] = total[:, c * members : (c + 1) * members]


def exchange(value, axis, bit):
    size = lax.axis_size(axis)
    return lax.ppermute(value, axis, [(i, i ^ bit) for i in range(size)])


def halve(chunks, tile, bit):
    mine = (tile // bit) % 2
    keeps, sends = [], []
    for keep, got in chunks:
        shape = (keep.shape[0] // 2, 2) + keep.shape[1:]
        keep, got = keep.reshape(shape), got.reshape(shape)
        for side, out in ((1 - mine, sends), (mine, keeps)):
            out.append(
                lax.dynamic_index_in_dim(keep, side, 1, False)
                + lax.dynamic_index_in_dim(got, side, 1, False)
            )
    return [(keep, exchange(send, "tile", bit)) for keep, send in zip(keeps, sends)]


ANY = pl.BlockSpec(memory_space=pl.ANY)
VMEM = pl.BlockSpec(memory_space=pltpu.MemorySpace.VMEM)
PARAMS = pltpu.CompilerParams(vmem_limit_bytes=16 * 1024 * 1024)
SMEM = pl.BlockSpec(memory_space=pltpu.MemorySpace.SMEM)


def local(
    northward_speed_field,
    level_depth_extent,
    potential_warmth_anomaly,
    ocean_region_label,
    zone_for_parallel,
):
    members_here, layers, columns, lats = northward_speed_field.shape
    tiles = lax.axis_size("tile")
    groups = lax.axis_size("member")
    members = members_here * groups
    per_block = LANES // SUB // tiles
    half = lats // LANES // 2
    count = groups // 2
    slots = members_here + 1
    assert lats == groups * tiles * SUB and groups * HEAT_LANES <= LANES
    assert half >= 1 and half * per_block == count and lats == 2 * half * LANES
    spacing = (metric_factor(lats) / math.sqrt(columns * tiles)).reshape(1, lats)
    rows = members_here * layers * columns
    sizes = dict(
        half=half, members_here=members_here, layers=layers, columns=columns,
        groups=groups, tiles=tiles,
    )
    blocked = [
        pltpu.with_memory_space_constraint(
            x.reshape(rows // columns, columns, 2 * half, LANES)
            .transpose(0, 2, 1, 3)
            .reshape(2 * half * rows, LANES),
            pltpu.MemorySpace.HBM,
        )
        for x in (northward_speed_field, level_depth_extent, potential_warmth_anomaly)
    ]
    labels = pltpu.with_memory_space_constraint(ocean_region_label, pltpu.MemorySpace.HBM)
    early = pltpu.VMEM((tiles // 2, count * slots, SUB, LANES), jnp.float32)
    late = pltpu.VMEM((tiles // 2, count * slots + 1, SUB, LANES), jnp.float32)
    keep0, send0, heat, data, labels = pl.pallas_call(
        functools.partial(first_kernel, **sizes),
        out_shape=(
            early,
            early,
            pltpu.VMEM((LANES, LANES), jnp.float32),
            pltpu.VMEM((3, 2 * half * rows, LANES), jnp.float32),
            pltpu.VMEM((columns, lats), jnp.int32),
        ),
        in_specs=[ANY] * 4 + [VMEM],
        out_specs=(VMEM,) * 5,
        scratch_shapes=[pltpu.SemaphoreType.DMA((3,)), pltpu.SemaphoreType.DMA(())],
        compiler_params=PARAMS,
        name="first",
    )(*blocked, labels, spacing)
    got0 = exchange(send0, "tile", 1)
    keep1, send1 = pl.pallas_call(
        functools.partial(second_kernel, **sizes),
        out_shape=(late, late),
        in_specs=[VMEM] * 4,
        out_specs=(VMEM, VMEM),
        compiler_params=PARAMS,
        name="second",
    )(data, labels, spacing, heat)
    got1 = exchange(send1, "tile", 1)
    bands = pl.pallas_call(
        functools.partial(bands_kernel, members=members, groups=groups, tiles=tiles),
        out_shape=pltpu.VMEM((groups, NBANDS * members, members * SUB), jnp.bfloat16),
        in_specs=[SMEM, ANY],
        out_specs=VMEM,
        compiler_params=PARAMS,
        name="bands",
    )(zone_for_parallel, got0)
    tile = lax.axis_index("tile")
    chunks = [(keep0, got0), (keep1, got1)]
    bit = 2
    while bit < tiles:
        chunks = halve(chunks, tile, bit)
        bit *= 2
    owned = jnp.concatenate([(keep + got)[0] for keep, got in chunks], 0)
    parts = [owned] + [exchange(owned, "member", r) for r in range(1, groups)]
    known = dict(members_here=members_here, layers=layers, groups=groups)
    share = pl.pallas_call(
        functools.partial(share_kernel, **known),
        out_shape=pltpu.VMEM((members, NBANDS * members), jnp.float32),
        in_specs=[VMEM] * (1 + groups),
        out_specs=VMEM,
        scratch_shapes=[pltpu.VMEM((groups, groups * slots, SUB, LANES), jnp.float32)],
        compiler_params=PARAMS,
        name="share",
    )(bands, *parts)
    psi, heat = pl.pallas_call(
        functools.partial(means_kernel, **known),
        out_shape=(
            jax.ShapeDtypeStruct((BASINS, SUB, layers), jnp.float32),
            jax.ShapeDtypeStruct((SUB, BASINS), jnp.float32),
        ),
        in_specs=[VMEM] * groups,
        out_specs=(VMEM, VMEM),
        compiler_params=PARAMS,
        name="means",
    )(*parts)
    bit = 1
    while 2 * bit < tiles:
        share = share + exchange(share, "tile", bit)
        bit *= 2
    norm = float((members - 1) * BASINS * layers * (lats // NBANDS))
    covariance = pl.pallas_call(
        functools.partial(unpack_kernel, members=members, scale=1.0 / norm),
        out_shape=jax.ShapeDtypeStruct((NBANDS, members, members), jnp.float32),
        in_specs=[VMEM] * 2,
        out_specs=VMEM,
        compiler_params=PARAMS,
        name="unpack",
    )(share, exchange(share, "tile", bit))
    return (jnp.transpose(psi, (0, 2, 1)), jnp.transpose(heat, (1, 0)), covariance)


def solution(mesh):
    in_specs = (
        P("member", None, "tile", None),
        P("member", None, "tile", None),
        P("member", None, "tile", None),
        P("tile", None),
        P(),
    )
    out_specs = (P(None, None, ("member", "tile")), P(None, ("member", "tile")), P())
    return jax.shard_map(local, mesh=mesh, in_specs=in_specs, out_specs=out_specs, check_vma=False)
```

```python
import functools
import math

import jax
import jax.numpy as jnp
from jax import lax
from jax.experimental import pallas as pl
from jax.experimental.pallas import tpu as pltpu
from jax.sharding import PartitionSpec as P


BASINS = 10
NBANDS = 16
LANES = 128
SUB = 8
HEAT_LANES = 16


def metric_factor(lats):
    index = jnp.arange(lats, dtype=jnp.float32)
    return jnp.cos((-80.0 + 160.0 * (index + 0.5) / lats) * (math.pi / 180.0))


def iota(shape, dim):
    return lax.broadcasted_iota(jnp.int32, shape, dim)


def log2(n):
    assert n & (n - 1) == 0
    return n.bit_length() - 1


def split_features(layers, members_here):
    feats = BASINS * layers
    rest = feats - LANES
    assert 0 < rest and rest * members_here == LANES and LANES % layers == 0
    return feats, rest


def exact_parts(x):
    parts = []
    for _ in range(3):
        parts.append(x.astype(jnp.bfloat16))
        x = x - parts[-1].astype(jnp.float32)
    return parts


def basin_sums(buf, region, spacing, heat_ref, keep_ref, send_ref,
               *, late, half, members_here, layers, columns, groups, tiles):
    feats, _ = split_features(layers, members_here)
    core = lax.axis_index("tile") % 2
    halves = layers // SUB
    lshift = log2(layers)
    slots = members_here + 1
    pieces = LANES // SUB
    blocks = 2 * half
    per = layers * blocks * columns
    mine = range(half, blocks) if late else range(half)
    rows = iota((feats, feats), 0)
    cols = iota((feats, feats), 1)
    running = ((rows >> lshift) == (cols >> lshift)) & (cols <= rows)
    running = jnp.where(running, 1.0, 0.0).astype(jnp.bfloat16)
    rows = iota((LANES, BASINS * SUB), 0)
    cols = iota((LANES, BASINS * SUB), 1)
    gather = jnp.where((rows & (HEAT_LANES - 1)) == (cols >> log2(SUB)), 1.0, 0.0)
    gather = gather.astype(jnp.bfloat16)
    heat_group = iota((LANES, LANES), 0) >> log2(HEAT_LANES)
    heat_lat = iota((LANES, LANES), 1)

    def select(table, x):
        return jnp.dot(
            jnp.concatenate([table] * 3, 1), jnp.concatenate(exact_parts(x), 0),
            preferred_element_type=jnp.float32,
        )

    def put(place, slot, even, odd):
        keep_ref[place, slot] = jnp.where(core == 0, even, odd)
        send_ref[place, slot] = jnp.where(core == 0, odd, even)

    def put_block(lb, s, value):
        for row in range(0, pieces, 2):
            group, tile = divmod(lb * pieces + row, tiles)
            slot = (group % (groups // 2)) * slots + s
            even = value[row * SUB : (row + 1) * SUB]
            put(tile // 2, slot, even, value[(row + 1) * SUB : (row + 2) * SUB])

    warm = [[None] * columns for _ in range(blocks)]
    extra = [[] for _ in range(blocks)]

    def label(lb, x):
        line = region[x : x + 1, lb * LANES : (lb + 1) * LANES]
        return jnp.broadcast_to(line, (SUB, LANES))

    for m in range(members_here):
        for lb in mine:
            scale = spacing[:, lb * LANES : (lb + 1) * LANES]
            acc = [[None] * halves for _ in range(BASINS)]
            for x in range(columns):
                flux = []
                for k in range(halves):
                    start = m * per + (k * SUB * blocks + lb) * columns + x
                    at = pl.ds(start, SUB, stride=blocks * columns)
                    one = buf[0, at, :] * buf[1, at, :] * scale
                    heat = one * buf[2, at, :]
                    warm[lb][x] = heat if warm[lb][x] is None else warm[lb][x] + heat
                    flux.append(one)
                here = label(lb, x)
                for b in range(BASINS):
                    hit = here == b
                    for k in range(halves):
                        part = jnp.where(hit, flux[k], 0.0)
                        acc[b][k] = part if acc[b][k] is None else acc[b][k] + part
            stacked = jnp.concatenate([acc[b][k] for b in range(BASINS) for k in range(halves)], 0)
            stream = select(running, stacked)
            put_block(lb, m, stream[:LANES].T)
            extra[lb].append(stream[LANES:])
    span = tiles * SUB
    heat = heat_ref[...] if late else None
    for lb in mine:
        put_block(lb, members_here, jnp.concatenate(extra[lb], 0).T)
        basin_heat = []
        for b in range(BASINS):
            total = None
            for x in range(columns):
                part = jnp.where(label(lb, x) == b, warm[lb][x], 0.0)
                total = part if total is None else total + part
            basin_heat.append(total)
        block = select(gather, jnp.concatenate(basin_heat, 0))
        for p in range(LANES // span):
            moved = block if p == 0 else pltpu.roll(block, LANES - p * span, 1)
            keep = (heat_group == lb * (LANES // span) + p) & (heat_lat < span)
            part = jnp.where(keep, moved, 0.0)
            heat = part if heat is None else heat + part
    if not late:
        heat_ref[...] = heat
        return
    heat = heat.T
    for t in range(0, tiles, 2):
        even = heat[t * SUB : (t + 1) * SUB]
        put(t // 2, slots * (groups // 2), even, heat[(t + 1) * SUB : (t + 2) * SUB])


def first_kernel(v_ref, h_ref, w_ref, region_ref, spacing_ref, keep_ref, send_ref, heat_ref,
                 data_ref, small_ref, sems, small_sem, **sizes):
    copies = [pltpu.make_async_copy(region_ref, small_ref, small_sem)]
    for a, ref in enumerate((v_ref, h_ref, w_ref)):
        copies.append(pltpu.make_async_copy(ref, data_ref.at[a], sems.at[a]))
    for copy in copies:
        copy.start(priority=1)
    for copy in copies:
        copy.wait()
    basin_sums(
        data_ref, small_ref[...], spacing_ref[...], heat_ref, keep_ref, send_ref,
        late=False, **sizes,
    )


def second_kernel(data_ref, region_ref, spacing_ref, heat_ref, keep_ref, send_ref, **sizes):
    basin_sums(
        data_ref, region_ref[...], spacing_ref[...], heat_ref, keep_ref, send_ref,
        late=True, **sizes,
    )


def bands_kernel(zone_ref, order_ref, out_ref, *, members, groups, tiles):
    tile = lax.axis_index("tile")
    wide = members * SUB
    sshift = log2(SUB)
    row = iota((NBANDS * members, wide), 0)
    col = iota((NBANDS * members, wide), 1)
    same_member = (row & (members - 1)) == (col >> sshift)
    band = row >> log2(members)
    lat_lane = iota((1, wide), 1) & (SUB - 1)
    for g in range(groups):
        zone = jnp.zeros((1, wide), jnp.int32)
        for j in range(SUB):
            zone = jnp.where(lat_lane == j, zone_ref[(g * tiles + tile) * SUB + j], zone)
        hit = jnp.where(same_member & (band == zone), 1.0, 0.0)
        out_ref[g] = hit.astype(jnp.bfloat16)


def share_kernel(*refs, members_here, layers, groups):
    bands_ref = refs[0]
    parts = refs[1 : 1 + groups]
    cov_ref, all_ref = refs[1 + groups :]
    _, rest = split_features(layers, members_here)
    slots = members_here + 1
    members = members_here * groups
    mine = lax.axis_index("member")
    for r in range(groups):
        all_ref[mine ^ r] = parts[r][: groups * slots]
    wide = members * SUB
    lane = iota((SUB, LANES), 1)
    jmask = SUB - 1
    same_lat = (iota((SUB, wide), 0)) == (iota((SUB, wide), 1) & jmask)
    last = (((1,), (1,)), ((), ()))
    total = None
    for g in range(groups):
        heads, tails = [], []
        for q in range(groups):
            tail = all_ref[q, g * slots + members_here]
            for m in range(members_here):
                heads.append(all_ref[q, g * slots + m])
                moved = tail if m == 0 else pltpu.roll(tail, LANES - m * rest, 1)
                tails.append(jnp.where(lane < rest, moved, 0.0))
        head_mean = sum(heads) * (1.0 / members)
        tail_mean = sum(tails) * (1.0 / members)
        head = jnp.concatenate([a - head_mean for a in heads], 0)
        tail = jnp.concatenate([a - tail_mean for a in tails], 0)
        both = jnp.concatenate([head, tail], 1)
        high = both.astype(jnp.bfloat16)
        low = (both - high.astype(jnp.float32)).astype(jnp.bfloat16)
        gram = lax.dot_general(
            jnp.concatenate([high, high, low], 1), jnp.concatenate([high, low, high], 1),
            last, preferred_element_type=jnp.float32,
        )
        summed = jnp.concatenate(
            [
                jnp.sum(
                    jnp.where(same_lat, gram[n * SUB : (n + 1) * SUB], 0.0), axis=0, keepdims=True
                )
                for n in range(members)
            ],
            0,
        )
        share = lax.dot_general(
            jnp.concatenate(exact_parts(summed), 0), bands_ref[g], last,
            preferred_element_type=jnp.float32,
        )
        total = share if total is None else total + share
    cov_ref[...] = total[:members] + (total[members : 2 * members] + total[2 * members :])


def means_kernel(*refs, members_here, layers, groups):
    parts = refs[:groups]
    psi_ref, heat_ref = refs[groups:]
    _, rest = split_features(layers, members_here)
    slots = members_here + 1
    members = members_here * groups
    mine = lax.axis_index("member")
    at = mine * slots

    def total(slot):
        return sum(ref[slot] for ref in parts)

    head = sum(total(at + m) for m in range(members_here)) * (1.0 / members)
    packed = total(at + members_here)
    tail = packed
    for m in range(1, members_here):
        tail = tail + pltpu.roll(packed, LANES - m * rest, 1)
    tail = tail * (1.0 / members)
    for b in range(BASINS):
        part, lane = divmod(b * layers, LANES)
        psi_ref[b] = (tail if part else head)[:, lane : lane + layers]
    warm = total(groups * slots)
    out = jnp.zeros((SUB, BASINS), jnp.float32)
    for g in range(groups):
        out = jnp.where(mine == g, warm[:, g * HEAT_LANES : g * HEAT_LANES + BASINS], out)
    heat_ref[...] = out * (1.0 / (members * math.sqrt(layers)))


def unpack_kernel(*refs, members, scale):
    out_ref = refs[-1]
    total = refs[0][...]
    for ref in refs[1:-1]:
        total = total + ref[...]
    total = total * scale
    for c in range(NBANDS):
        out_ref[c] = total[:, c * members : (c + 1) * members]


def exchange(value, axis, bit):
    size = lax.axis_size(axis)
    return lax.ppermute(value, axis, [(i, i ^ bit) for i in range(size)])


def sum_stages(tiles):
    stages, size = [(3, 2, 1)], 4
    while size < tiles:
        stages.append((size,))
        size *= 2
    return stages


def halve(chunks, tile, bit):
    mine = (tile // bit) % 2
    keeps, sends = [], []
    for keep, got in chunks:
        shape = (keep.shape[0] // 2, 2) + keep.shape[1:]
        keep, got = keep.reshape(shape), got.reshape(shape)
        for side, out in ((1 - mine, sends), (mine, keeps)):
            out.append(
                lax.dynamic_index_in_dim(keep, side, 1, False)
                + lax.dynamic_index_in_dim(got, side, 1, False)
            )
    return [(keep, exchange(send, "tile", bit)) for keep, send in zip(keeps, sends)]


ANY = pl.BlockSpec(memory_space=pl.ANY)
VMEM = pl.BlockSpec(memory_space=pltpu.MemorySpace.VMEM)
PARAMS = pltpu.CompilerParams(vmem_limit_bytes=16 * 1024 * 1024)
SMEM = pl.BlockSpec(memory_space=pltpu.MemorySpace.SMEM)


def local(
    northward_speed_field,
    level_depth_extent,
    potential_warmth_anomaly,
    ocean_region_label,
    zone_for_parallel,
):
    members_here, layers, columns, lats = northward_speed_field.shape
    tiles = lax.axis_size("tile")
    groups = lax.axis_size("member")
    members = members_here * groups
    per_block = LANES // SUB // tiles
    half = lats // LANES // 2
    count = groups // 2
    slots = members_here + 1
    assert lats == groups * tiles * SUB and groups * HEAT_LANES <= LANES
    assert half >= 1 and half * per_block == count and lats == 2 * half * LANES
    spacing = (metric_factor(lats) / math.sqrt(columns * tiles)).reshape(1, lats)
    rows = members_here * layers * columns
    sizes = dict(
        half=half, members_here=members_here, layers=layers, columns=columns,
        groups=groups, tiles=tiles,
    )
    blocked = [
        pltpu.with_memory_space_constraint(
            x.reshape(rows // columns, columns, 2 * half, LANES)
            .transpose(0, 2, 1, 3)
            .reshape(2 * half * rows, LANES),
            pltpu.MemorySpace.HBM,
        )
        for x in (northward_speed_field, level_depth_extent, potential_warmth_anomaly)
    ]
    labels = pltpu.with_memory_space_constraint(ocean_region_label, pltpu.MemorySpace.HBM)
    early = pltpu.VMEM((tiles // 2, count * slots, SUB, LANES), jnp.float32)
    late = pltpu.VMEM((tiles // 2, count * slots + 1, SUB, LANES), jnp.float32)
    keep0, send0, heat, data, labels = pl.pallas_call(
        functools.partial(first_kernel, **sizes),
        out_shape=(
            early,
            early,
            pltpu.VMEM((LANES, LANES), jnp.float32),
            pltpu.VMEM((3, 2 * half * rows, LANES), jnp.float32),
            pltpu.VMEM((columns, lats), jnp.int32),
        ),
        in_specs=[ANY] * 4 + [VMEM],
        out_specs=(VMEM,) * 5,
        scratch_shapes=[pltpu.SemaphoreType.DMA((3,)), pltpu.SemaphoreType.DMA(())],
        compiler_params=PARAMS,
        name="first",
    )(*blocked, labels, spacing)
    got0 = exchange(send0, "tile", 1)
    keep1, send1 = pl.pallas_call(
        functools.partial(second_kernel, **sizes),
        out_shape=(late, late),
        in_specs=[VMEM] * 4,
        out_specs=(VMEM, VMEM),
        compiler_params=PARAMS,
        name="second",
    )(data, labels, spacing, heat)
    got1 = exchange(send1, "tile", 1)
    bands = pl.pallas_call(
        functools.partial(bands_kernel, members=members, groups=groups, tiles=tiles),
        out_shape=pltpu.VMEM((groups, NBANDS * members, members * SUB), jnp.bfloat16),
        in_specs=[SMEM, ANY],
        out_specs=VMEM,
        compiler_params=PARAMS,
        name="bands",
    )(zone_for_parallel, got0)
    tile = lax.axis_index("tile")
    chunks = [(keep0, got0), (keep1, got1)]
    bit = 2
    while bit < tiles:
        chunks = halve(chunks, tile, bit)
        bit *= 2
    owned = jnp.concatenate([(keep + got)[0] for keep, got in chunks], 0)
    parts = [owned] + [exchange(owned, "member", r) for r in range(1, groups)]
    known = dict(members_here=members_here, layers=layers, groups=groups)
    share = pl.pallas_call(
        functools.partial(share_kernel, **known),
        out_shape=pltpu.VMEM((members, NBANDS * members), jnp.float32),
        in_specs=[VMEM] * (1 + groups),
        out_specs=VMEM,
        scratch_shapes=[pltpu.VMEM((groups, groups * slots, SUB, LANES), jnp.float32)],
        compiler_params=PARAMS,
        name="share",
    )(bands, *parts)
    psi, heat = pl.pallas_call(
        functools.partial(means_kernel, **known),
        out_shape=(
            jax.ShapeDtypeStruct((BASINS, SUB, layers), jnp.float32),
            jax.ShapeDtypeStruct((SUB, BASINS), jnp.float32),
        ),
        in_specs=[VMEM] * groups,
        out_specs=(VMEM, VMEM),
        compiler_params=PARAMS,
        name="means",
    )(*parts)
    norm = float((members - 1) * BASINS * layers * (lats // NBANDS))
    stages = sum_stages(tiles)
    for stage in stages[:-1]:
        gots = [exchange(share, "tile", r) for r in stage]
        for got in gots:
            share = share + got
    gots = [exchange(share, "tile", r) for r in stages[-1]]
    covariance = pl.pallas_call(
        functools.partial(unpack_kernel, members=members, scale=1.0 / norm),
        out_shape=jax.ShapeDtypeStruct((NBANDS, members, members), jnp.float32),
        in_specs=[VMEM] * (1 + len(gots)),
        out_specs=VMEM,
        compiler_params=PARAMS,
        name="unpack",
    )(share, *gots)
    return (jnp.transpose(psi, (0, 2, 1)), jnp.transpose(heat, (1, 0)), covariance)


def solution(mesh):
    in_specs = (
        P("member", None, "tile", None),
        P("member", None, "tile", None),
        P("member", None, "tile", None),
        P("tile", None),
        P(),
    )
    out_specs = (P(None, None, ("member", "tile")), P(None, ("member", "tile")), P())
    return jax.shard_map(local, mesh=mesh, in_specs=in_specs, out_specs=out_specs, check_vma=False)
```

```python
import functools
import math

import jax
import jax.numpy as jnp
from jax import lax
from jax.experimental import pallas as pl
from jax.experimental.pallas import tpu as pltpu
from jax.sharding import PartitionSpec as P


BASINS = 10
NBANDS = 16
LANES = 128
SUB = 8
HEAT_LANES = 16


def metric_factor(lats):
    index = jnp.arange(lats, dtype=jnp.float32)
    return jnp.cos((-80.0 + 160.0 * (index + 0.5) / lats) * (math.pi / 180.0))


def iota(shape, dim):
    return lax.broadcasted_iota(jnp.int32, shape, dim)


def log2(n):
    assert n & (n - 1) == 0
    return n.bit_length() - 1


def split_features(layers, members_here):
    feats = BASINS * layers
    rest = feats - LANES
    assert 0 < rest and rest * members_here == LANES and LANES % layers == 0
    return feats, rest


def exact_parts(x):
    parts = []
    for _ in range(3):
        parts.append(x.astype(jnp.bfloat16))
        x = x - parts[-1].astype(jnp.float32)
    return parts


def basin_sums(buf, mask_ref, spacing, heat_ref, keep_ref, send_ref, wait,
               *, late, half, members_here, layers, columns, groups, tiles):
    feats, _ = split_features(layers, members_here)
    core = lax.axis_index("tile") % 2
    halves = layers // SUB
    lshift = log2(layers)
    slots = members_here + 1
    pieces = LANES // SUB
    blocks = 2 * half
    per = layers * blocks * columns
    mine = range(half, blocks) if late else range(half)
    rows = iota((feats, feats), 0)
    cols = iota((feats, feats), 1)
    running = ((rows >> lshift) == (cols >> lshift)) & (cols <= rows)
    running = jnp.where(running, 1.0, 0.0).astype(jnp.bfloat16)
    rows = iota((LANES, BASINS * SUB), 0)
    cols = iota((LANES, BASINS * SUB), 1)
    gather = jnp.where((rows & (HEAT_LANES - 1)) == (cols >> log2(SUB)), 1.0, 0.0)
    gather = gather.astype(jnp.bfloat16)
    heat_group = iota((LANES, LANES), 0) >> log2(HEAT_LANES)
    heat_lat = iota((LANES, LANES), 1)

    def select(table, x):
        return jnp.dot(
            jnp.concatenate([table] * 3, 1), jnp.concatenate(exact_parts(x), 0),
            preferred_element_type=jnp.float32,
        )

    def put(place, slot, even, odd):
        keep_ref[place, slot] = jnp.where(core == 0, even, odd)
        send_ref[place, slot] = jnp.where(core == 0, odd, even)

    def put_block(lb, s, value):
        for row in range(0, pieces, 2):
            group, tile = divmod(lb * pieces + row, tiles)
            slot = (group % (groups // 2)) * slots + s
            even = value[row * SUB : (row + 1) * SUB]
            put(tile // 2, slot, even, value[(row + 1) * SUB : (row + 2) * SUB])

    warm = [[None] * columns for _ in range(blocks)]
    extra = [[] for _ in range(blocks)]

    wait()
    for m in range(members_here):
        for lb in mine:
            scale = spacing[:, lb * LANES : (lb + 1) * LANES]
            acc = [[None] * halves for _ in range(BASINS)]
            for x in range(columns):
                flux = []
                for k in range(halves):
                    start = m * per + (k * SUB * blocks + lb) * columns + x
                    at = pl.ds(start, SUB, stride=blocks * columns)
                    one = buf[0, at, :] * buf[1, at, :] * scale
                    heat = one * buf[2, at, :]
                    warm[lb][x] = heat if warm[lb][x] is None else warm[lb][x] + heat
                    flux.append(one)
                for b in range(BASINS):
                    hit = mask_ref[lb, b, x]
                    for k in range(halves):
                        part = flux[k] * hit
                        acc[b][k] = part if acc[b][k] is None else acc[b][k] + part
            stacked = jnp.concatenate([acc[b][k] for b in range(BASINS) for k in range(halves)], 0)
            stream = select(running, stacked)
            put_block(lb, m, stream[:LANES].T)
            extra[lb].append(stream[LANES:])
    span = tiles * SUB
    heat = heat_ref[...] if late else None
    for lb in mine:
        put_block(lb, members_here, jnp.concatenate(extra[lb], 0).T)
        basin_heat = []
        for b in range(BASINS):
            total = None
            for x in range(columns):
                part = warm[lb][x] * mask_ref[lb, b, x]
                total = part if total is None else total + part
            basin_heat.append(total)
        block = select(gather, jnp.concatenate(basin_heat, 0))
        for p in range(LANES // span):
            moved = block if p == 0 else pltpu.roll(block, LANES - p * span, 1)
            keep = (heat_group == lb * (LANES // span) + p) & (heat_lat < span)
            part = jnp.where(keep, moved, 0.0)
            heat = part if heat is None else heat + part
    if not late:
        heat_ref[...] = heat
        return
    heat = heat.T
    for t in range(0, tiles, 2):
        even = heat[t * SUB : (t + 1) * SUB]
        put(t // 2, slots * (groups // 2), even, heat[(t + 1) * SUB : (t + 2) * SUB])


def first_kernel(v_ref, h_ref, w_ref, region_ref, spacing_ref, keep_ref, send_ref, heat_ref,
                 data_ref, mask_ref, small, sems, small_sem, **sizes):
    labels = pltpu.make_async_copy(region_ref, small, small_sem)
    labels.start()
    copies = []
    for a, ref in enumerate((v_ref, h_ref, w_ref)):
        copies.append(pltpu.make_async_copy(ref, data_ref.at[a], sems.at[a]))
        copies[-1].start()
    labels.wait()
    region = small[...]
    for lb in range(2 * sizes["half"]):
        for x in range(sizes["columns"]):
            line = region[x : x + 1, lb * LANES : (lb + 1) * LANES]
            label = jnp.broadcast_to(line, (SUB, LANES))
            for b in range(BASINS):
                mask_ref[lb, b, x] = jnp.where(label == b, 1.0, 0.0)

    def wait():
        for copy in copies:
            copy.wait()

    basin_sums(
        data_ref, mask_ref, spacing_ref[...], heat_ref, keep_ref, send_ref, wait,
        late=False, **sizes,
    )


def second_kernel(data_ref, mask_ref, spacing_ref, heat_ref, keep_ref, send_ref, **sizes):
    basin_sums(
        data_ref, mask_ref, spacing_ref[...], heat_ref, keep_ref, send_ref, lambda: None,
        late=True, **sizes,
    )


def bands_kernel(zone_ref, order_ref, out_ref, *, members, groups, tiles):
    tile = lax.axis_index("tile")
    wide = members * SUB
    sshift = log2(SUB)
    row = iota((NBANDS * members, wide), 0)
    col = iota((NBANDS * members, wide), 1)
    same_member = (row & (members - 1)) == (col >> sshift)
    band = row >> log2(members)
    lat_lane = iota((1, wide), 1) & (SUB - 1)
    for g in range(groups):
        zone = jnp.zeros((1, wide), jnp.int32)
        for j in range(SUB):
            zone = jnp.where(lat_lane == j, zone_ref[(g * tiles + tile) * SUB + j], zone)
        hit = jnp.where(same_member & (band == zone), 1.0, 0.0)
        out_ref[g] = hit.astype(jnp.bfloat16)


def share_kernel(*refs, members_here, layers, groups):
    bands_ref = refs[0]
    parts = refs[1 : 1 + groups]
    cov_ref, all_ref = refs[1 + groups :]
    _, rest = split_features(layers, members_here)
    slots = members_here + 1
    members = members_here * groups
    mine = lax.axis_index("member")
    for r in range(groups):
        all_ref[mine ^ r] = parts[r][: groups * slots]
    wide = members * SUB
    lane = iota((SUB, LANES), 1)
    jmask = SUB - 1
    same_lat = (iota((SUB, wide), 0)) == (iota((SUB, wide), 1) & jmask)
    last = (((1,), (1,)), ((), ()))
    total = None
    for g in range(groups):
        heads, tails = [], []
        for q in range(groups):
            tail = all_ref[q, g * slots + members_here]
            for m in range(members_here):
                heads.append(all_ref[q, g * slots + m])
                moved = tail if m == 0 else pltpu.roll(tail, LANES - m * rest, 1)
                tails.append(jnp.where(lane < rest, moved, 0.0))
        head_mean = sum(heads) * (1.0 / members)
        tail_mean = sum(tails) * (1.0 / members)
        head = jnp.concatenate([a - head_mean for a in heads], 0)
        tail = jnp.concatenate([a - tail_mean for a in tails], 0)
        both = jnp.concatenate([head, tail], 1)
        high = both.astype(jnp.bfloat16)
        low = (both - high.astype(jnp.float32)).astype(jnp.bfloat16)
        gram = lax.dot_general(
            jnp.concatenate([high, high, low], 1), jnp.concatenate([high, low, high], 1),
            last, preferred_element_type=jnp.float32,
        )
        summed = jnp.concatenate(
            [
                jnp.sum(
                    jnp.where(same_lat, gram[n * SUB : (n + 1) * SUB], 0.0), axis=0, keepdims=True
                )
                for n in range(members)
            ],
            0,
        )
        share = lax.dot_general(
            jnp.concatenate(exact_parts(summed), 0), bands_ref[g], last,
            preferred_element_type=jnp.float32,
        )
        total = share if total is None else total + share
    cov_ref[...] = total[:members] + (total[members : 2 * members] + total[2 * members :])


def means_kernel(*refs, members_here, layers, groups):
    parts = refs[:groups]
    psi_ref, heat_ref = refs[groups:]
    _, rest = split_features(layers, members_here)
    slots = members_here + 1
    members = members_here * groups
    mine = lax.axis_index("member")
    at = mine * slots

    def total(slot):
        return sum(ref[slot] for ref in parts)

    head = sum(total(at + m) for m in range(members_here)) * (1.0 / members)
    packed = total(at + members_here)
    tail = packed
    for m in range(1, members_here):
        tail = tail + pltpu.roll(packed, LANES - m * rest, 1)
    tail = tail * (1.0 / members)
    for b in range(BASINS):
        part, lane = divmod(b * layers, LANES)
        psi_ref[b] = (tail if part else head)[:, lane : lane + layers]
    warm = total(groups * slots)
    out = jnp.zeros((SUB, BASINS), jnp.float32)
    for g in range(groups):
        out = jnp.where(mine == g, warm[:, g * HEAT_LANES : g * HEAT_LANES + BASINS], out)
    heat_ref[...] = out * (1.0 / (members * math.sqrt(layers)))


def unpack_kernel(*refs, members, scale):
    out_ref = refs[-1]
    total = refs[0][...]
    for ref in refs[1:-1]:
        total = total + ref[...]
    total = total * scale
    for c in range(NBANDS):
        out_ref[c] = total[:, c * members : (c + 1) * members]


def exchange(value, axis, bit):
    size = lax.axis_size(axis)
    return lax.ppermute(value, axis, [(i, i ^ bit) for i in range(size)])


def sum_stages(tiles):
    stages, size = [(3, 2, 1)], 4
    while size < tiles:
        stages.append((size,))
        size *= 2
    return stages


def halve(chunks, tile, bit):
    mine = (tile // bit) % 2
    keeps, sends = [], []
    for keep, got in chunks:
        shape = (keep.shape[0] // 2, 2) + keep.shape[1:]
        keep, got = keep.reshape(shape), got.reshape(shape)
        for side, out in ((1 - mine, sends), (mine, keeps)):
            out.append(
                lax.dynamic_index_in_dim(keep, side, 1, False)
                + lax.dynamic_index_in_dim(got, side, 1, False)
            )
    return [(keep, exchange(send, "tile", bit)) for keep, send in zip(keeps, sends)]


ANY = pl.BlockSpec(memory_space=pl.ANY)
VMEM = pl.BlockSpec(memory_space=pltpu.MemorySpace.VMEM)
PARAMS = pltpu.CompilerParams(vmem_limit_bytes=16 * 1024 * 1024)
SMEM = pl.BlockSpec(memory_space=pltpu.MemorySpace.SMEM)


def local(
    northward_speed_field,
    level_depth_extent,
    potential_warmth_anomaly,
    ocean_region_label,
    zone_for_parallel,
):
    members_here, layers, columns, lats = northward_speed_field.shape
    tiles = lax.axis_size("tile")
    groups = lax.axis_size("member")
    members = members_here * groups
    per_block = LANES // SUB // tiles
    half = lats // LANES // 2
    count = groups // 2
    slots = members_here + 1
    assert lats == groups * tiles * SUB and groups * HEAT_LANES <= LANES
    assert half >= 1 and half * per_block == count and lats == 2 * half * LANES
    spacing = (metric_factor(lats) / math.sqrt(columns * tiles)).reshape(1, lats)
    rows = members_here * layers * columns
    sizes = dict(
        half=half, members_here=members_here, layers=layers, columns=columns,
        groups=groups, tiles=tiles,
    )
    blocked = [
        pltpu.with_memory_space_constraint(
            x.reshape(rows // columns, columns, 2 * half, LANES)
            .transpose(0, 2, 1, 3)
            .reshape(2 * half * rows, LANES),
            pltpu.MemorySpace.HBM,
        )
        for x in (northward_speed_field, level_depth_extent, potential_warmth_anomaly)
    ]
    labels = pltpu.with_memory_space_constraint(ocean_region_label, pltpu.MemorySpace.HBM)
    early = pltpu.VMEM((tiles // 2, count * slots, SUB, LANES), jnp.float32)
    late = pltpu.VMEM((tiles // 2, count * slots + 1, SUB, LANES), jnp.float32)
    keep0, send0, heat, data, mask = pl.pallas_call(
        functools.partial(first_kernel, **sizes),
        out_shape=(
            early,
            early,
            pltpu.VMEM((LANES, LANES), jnp.float32),
            pltpu.VMEM((3, 2 * half * rows, LANES), jnp.float32),
            pltpu.VMEM((2 * half, BASINS, columns, SUB, LANES), jnp.float32),
        ),
        in_specs=[ANY] * 4 + [VMEM],
        out_specs=(VMEM,) * 5,
        scratch_shapes=[
            pltpu.VMEM((columns, lats), jnp.int32),
            pltpu.SemaphoreType.DMA((3,)),
            pltpu.SemaphoreType.DMA(()),
        ],
        compiler_params=PARAMS,
        name="first",
    )(*blocked, labels, spacing)
    got0 = exchange(send0, "tile", 1)
    keep1, send1 = pl.pallas_call(
        functools.partial(second_kernel, **sizes),
        out_shape=(late, late),
        in_specs=[VMEM] * 4,
        out_specs=(VMEM, VMEM),
        compiler_params=PARAMS,
        name="second",
    )(data, mask, spacing, heat)
    got1 = exchange(send1, "tile", 1)
    bands = pl.pallas_call(
        functools.partial(bands_kernel, members=members, groups=groups, tiles=tiles),
        out_shape=pltpu.VMEM((groups, NBANDS * members, members * SUB), jnp.bfloat16),
        in_specs=[SMEM, ANY],
        out_specs=VMEM,
        compiler_params=PARAMS,
        name="bands",
    )(zone_for_parallel, got0)
    tile = lax.axis_index("tile")
    chunks = [(keep0, got0), (keep1, got1)]
    bit = 2
    while bit < tiles:
        chunks = halve(chunks, tile, bit)
        bit *= 2
    owned = jnp.concatenate([(keep + got)[0] for keep, got in chunks], 0)
    parts = [owned] + [exchange(owned, "member", r) for r in range(1, groups)]
    known = dict(members_here=members_here, layers=layers, groups=groups)
    share = pl.pallas_call(
        functools.partial(share_kernel, **known),
        out_shape=pltpu.VMEM((members, NBANDS * members), jnp.float32),
        in_specs=[VMEM] * (1 + groups),
        out_specs=VMEM,
        scratch_shapes=[pltpu.VMEM((groups, groups * slots, SUB, LANES), jnp.float32)],
        compiler_params=PARAMS,
        name="share",
    )(bands, *parts)
    psi, heat = pl.pallas_call(
        functools.partial(means_kernel, **known),
        out_shape=(
            jax.ShapeDtypeStruct((BASINS, SUB, layers), jnp.float32),
            jax.ShapeDtypeStruct((SUB, BASINS), jnp.float32),
        ),
        in_specs=[VMEM] * groups,
        out_specs=(VMEM, VMEM),
        compiler_params=PARAMS,
        name="means",
    )(*parts)
    norm = float((members - 1) * BASINS * layers * (lats // NBANDS))
    stages = sum_stages(tiles)
    for stage in stages[:-1]:
        gots = [exchange(share, "tile", r) for r in stage]
        for got in gots:
            share = share + got
    gots = [exchange(share, "tile", r) for r in stages[-1]]
    covariance = pl.pallas_call(
        functools.partial(unpack_kernel, members=members, scale=1.0 / norm),
        out_shape=jax.ShapeDtypeStruct((NBANDS, members, members), jnp.float32),
        in_specs=[VMEM] * (1 + len(gots)),
        out_specs=VMEM,
        compiler_params=PARAMS,
        name="unpack",
    )(share, *gots)
    return (jnp.transpose(psi, (0, 2, 1)), jnp.transpose(heat, (1, 0)), covariance)


def solution(mesh):
    in_specs = (
        P("member", None, "tile", None),
        P("member", None, "tile", None),
        P("member", None, "tile", None),
        P("tile", None),
        P(),
    )
    out_specs = (P(None, None, ("member", "tile")), P(None, ("member", "tile")), P())
    return jax.shard_map(local, mesh=mesh, in_specs=in_specs, out_specs=out_specs, check_vma=False)
```

```python
import functools
import math

import jax
import jax.numpy as jnp
from jax import lax
from jax.experimental import pallas as pl
from jax.experimental.pallas import tpu as pltpu
from jax.sharding import PartitionSpec as P


BASINS = 10
NBANDS = 16
LANES = 128
SUB = 8
HEAT_LANES = 16


def iota(shape, dim):
    return lax.broadcasted_iota(jnp.int32, shape, dim)


def log2(n):
    assert n & (n - 1) == 0
    return n.bit_length() - 1


def split_features(layers, members_here):
    feats = BASINS * layers
    rest = feats - LANES
    assert 0 < rest and rest * members_here == LANES and LANES % layers == 0
    return feats, rest


def exact_parts(x):
    parts = []
    for _ in range(3):
        parts.append(x.astype(jnp.bfloat16))
        x = x - parts[-1].astype(jnp.float32)
    return parts


def basin_sums(buf, mask_ref, spacing, heat_ref, keep_ref, send_ref, wait,
               *, late, half, members_here, layers, columns, groups, tiles):
    feats, _ = split_features(layers, members_here)
    core = lax.axis_index("tile") % 2
    halves = layers // SUB
    lshift = log2(layers)
    slots = members_here + 1
    pieces = LANES // SUB
    blocks = 2 * half
    per = layers * blocks * columns
    mine = range(half, blocks) if late else range(half)
    rows = iota((feats, feats), 0)
    cols = iota((feats, feats), 1)
    running = ((rows >> lshift) == (cols >> lshift)) & (cols <= rows)
    running = jnp.where(running, 1.0, 0.0).astype(jnp.bfloat16)
    rows = iota((LANES, BASINS * SUB), 0)
    cols = iota((LANES, BASINS * SUB), 1)
    gather = jnp.where((rows & (HEAT_LANES - 1)) == (cols >> log2(SUB)), 1.0, 0.0)
    gather = gather.astype(jnp.bfloat16)
    heat_group = iota((LANES, LANES), 0) >> log2(HEAT_LANES)
    heat_lat = iota((LANES, LANES), 1)

    def select(table, x):
        return jnp.dot(
            jnp.concatenate([table] * 3, 1), jnp.concatenate(exact_parts(x), 0),
            preferred_element_type=jnp.float32,
        )

    def put(place, slot, even, odd):
        keep_ref[place, slot] = jnp.where(core == 0, even, odd)
        send_ref[place, slot] = jnp.where(core == 0, odd, even)

    def put_block(lb, s, value):
        for row in range(0, pieces, 2):
            group, tile = divmod(lb * pieces + row, tiles)
            slot = (group % (groups // 2)) * slots + s
            even = value[row * SUB : (row + 1) * SUB]
            put(tile // 2, slot, even, value[(row + 1) * SUB : (row + 2) * SUB])

    warm = [[None] * columns for _ in range(blocks)]
    extra = [[] for _ in range(blocks)]

    wait()
    for m in range(members_here):
        for lb in mine:
            scale = spacing[:, lb * LANES : (lb + 1) * LANES]
            acc = [[None] * halves for _ in range(BASINS)]
            for x in range(columns):
                flux = []
                for k in range(halves):
                    start = m * per + (k * SUB * blocks + lb) * columns + x
                    at = pl.ds(start, SUB, stride=blocks * columns)
                    one = buf[0, at, :] * buf[1, at, :] * scale
                    heat = one * buf[2, at, :]
                    warm[lb][x] = heat if warm[lb][x] is None else warm[lb][x] + heat
                    flux.append(one)
                for b in range(BASINS):
                    hit = mask_ref[lb, b, x]
                    for k in range(halves):
                        part = flux[k] * hit
                        acc[b][k] = part if acc[b][k] is None else acc[b][k] + part
            stacked = jnp.concatenate([acc[b][k] for b in range(BASINS) for k in range(halves)], 0)
            stream = select(running, stacked)
            put_block(lb, m, stream[:LANES].T)
            extra[lb].append(stream[LANES:])
    span = tiles * SUB
    heat = heat_ref[...] if late else None
    for lb in mine:
        put_block(lb, members_here, jnp.concatenate(extra[lb], 0).T)
        basin_heat = []
        for b in range(BASINS):
            total = None
            for x in range(columns):
                part = warm[lb][x] * mask_ref[lb, b, x]
                total = part if total is None else total + part
            basin_heat.append(total)
        block = select(gather, jnp.concatenate(basin_heat, 0))
        for p in range(LANES // span):
            moved = block if p == 0 else pltpu.roll(block, LANES - p * span, 1)
            keep = (heat_group == lb * (LANES // span) + p) & (heat_lat < span)
            part = jnp.where(keep, moved, 0.0)
            heat = part if heat is None else heat + part
    if not late:
        heat_ref[...] = heat
        return
    heat = heat.T
    for t in range(0, tiles, 2):
        even = heat[t * SUB : (t + 1) * SUB]
        put(t // 2, slots * (groups // 2), even, heat[(t + 1) * SUB : (t + 2) * SUB])


def first_kernel(v_ref, h_ref, w_ref, region_ref, keep_ref, send_ref, heat_ref,
                 data_ref, mask_ref, spacing_ref, small, sems, small_sem, **sizes):
    labels = pltpu.make_async_copy(region_ref, small, small_sem)
    labels.start()
    copies = []
    for a, ref in enumerate((v_ref, h_ref, w_ref)):
        copies.append(pltpu.make_async_copy(ref, data_ref.at[a], sems.at[a]))
        copies[-1].start()
    lats = spacing_ref.shape[1]
    index = iota(spacing_ref.shape, 1).astype(jnp.float32)
    angle = (-80.0 + 160.0 * (index + 0.5) / lats) * (math.pi / 180.0)
    spacing_ref[...] = jnp.cos(angle) * (1.0 / math.sqrt(sizes["columns"] * sizes["tiles"]))
    labels.wait()
    region = small[...]
    for lb in range(2 * sizes["half"]):
        for x in range(sizes["columns"]):
            line = region[x : x + 1, lb * LANES : (lb + 1) * LANES]
            label = jnp.broadcast_to(line, (SUB, LANES))
            for b in range(BASINS):
                mask_ref[lb, b, x] = jnp.where(label == b, 1.0, 0.0)

    def wait():
        for copy in copies:
            copy.wait()

    basin_sums(
        data_ref, mask_ref, spacing_ref[...], heat_ref, keep_ref, send_ref, wait,
        late=False, **sizes,
    )


def second_kernel(data_ref, mask_ref, spacing_ref, heat_ref, keep_ref, send_ref, **sizes):
    basin_sums(
        data_ref, mask_ref, spacing_ref[...], heat_ref, keep_ref, send_ref, lambda: None,
        late=True, **sizes,
    )


def bands_kernel(zone_ref, order_ref, out_ref, *, members, groups, tiles):
    tile = lax.axis_index("tile")
    wide = members * SUB
    sshift = log2(SUB)
    row = iota((NBANDS * members, wide), 0)
    col = iota((NBANDS * members, wide), 1)
    same_member = (row & (members - 1)) == (col >> sshift)
    band = row >> log2(members)
    lat_lane = iota((1, wide), 1) & (SUB - 1)
    for g in range(groups):
        zone = jnp.zeros((1, wide), jnp.int32)
        for j in range(SUB):
            zone = jnp.where(lat_lane == j, zone_ref[(g * tiles + tile) * SUB + j], zone)
        hit = jnp.where(same_member & (band == zone), 1.0, 0.0)
        out_ref[g] = hit.astype(jnp.bfloat16)


def share_kernel(*refs, members_here, layers, groups):
    bands_ref = refs[0]
    parts = refs[1 : 1 + groups]
    cov_ref, all_ref = refs[1 + groups :]
    _, rest = split_features(layers, members_here)
    slots = members_here + 1
    members = members_here * groups
    mine = lax.axis_index("member")
    for r in range(groups):
        all_ref[mine ^ r] = parts[r][: groups * slots]
    wide = members * SUB
    lane = iota((SUB, LANES), 1)
    jmask = SUB - 1
    same_lat = (iota((SUB, wide), 0)) == (iota((SUB, wide), 1) & jmask)
    last = (((1,), (1,)), ((), ()))
    total = None
    for g in range(groups):
        heads, tails = [], []
        for q in range(groups):
            tail = all_ref[q, g * slots + members_here]
            for m in range(members_here):
                heads.append(all_ref[q, g * slots + m])
                moved = tail if m == 0 else pltpu.roll(tail, LANES - m * rest, 1)
                tails.append(jnp.where(lane < rest, moved, 0.0))
        head_mean = sum(heads) * (1.0 / members)
        tail_mean = sum(tails) * (1.0 / members)
        head = jnp.concatenate([a - head_mean for a in heads], 0)
        tail = jnp.concatenate([a - tail_mean for a in tails], 0)
        both = jnp.concatenate([head, tail], 1)
        high = both.astype(jnp.bfloat16)
        low = (both - high.astype(jnp.float32)).astype(jnp.bfloat16)
        gram = lax.dot_general(
            jnp.concatenate([high, high, low], 1), jnp.concatenate([high, low, high], 1),
            last, preferred_element_type=jnp.float32,
        )
        summed = jnp.concatenate(
            [
                jnp.sum(
                    jnp.where(same_lat, gram[n * SUB : (n + 1) * SUB], 0.0), axis=0, keepdims=True
                )
                for n in range(members)
            ],
            0,
        )
        share = lax.dot_general(
            jnp.concatenate(exact_parts(summed), 0), bands_ref[g], last,
            preferred_element_type=jnp.float32,
        )
        total = share if total is None else total + share
    cov_ref[...] = total[:members] + (total[members : 2 * members] + total[2 * members :])


def means_kernel(*refs, members_here, layers, groups):
    parts = refs[:groups]
    psi_ref, heat_ref = refs[groups:]
    _, rest = split_features(layers, members_here)
    slots = members_here + 1
    members = members_here * groups
    mine = lax.axis_index("member")
    at = mine * slots

    def total(slot):
        return sum(ref[slot] for ref in parts)

    head = sum(total(at + m) for m in range(members_here)) * (1.0 / members)
    packed = total(at + members_here)
    tail = packed
    for m in range(1, members_here):
        tail = tail + pltpu.roll(packed, LANES - m * rest, 1)
    tail = tail * (1.0 / members)
    for b in range(BASINS):
        part, lane = divmod(b * layers, LANES)
        psi_ref[b] = (tail if part else head)[:, lane : lane + layers]
    warm = total(groups * slots)
    out = jnp.zeros((SUB, BASINS), jnp.float32)
    for g in range(groups):
        out = jnp.where(mine == g, warm[:, g * HEAT_LANES : g * HEAT_LANES + BASINS], out)
    heat_ref[...] = out * (1.0 / (members * math.sqrt(layers)))


def unpack_kernel(*refs, members, scale):
    out_ref = refs[-1]
    total = refs[0][...]
    for ref in refs[1:-1]:
        total = total + ref[...]
    total = total * scale
    for c in range(NBANDS):
        out_ref[c] = total[:, c * members : (c + 1) * members]


def exchange(value, axis, bit):
    size = lax.axis_size(axis)
    return lax.ppermute(value, axis, [(i, i ^ bit) for i in range(size)])


def sum_stages(tiles):
    stages, size = [(3, 2, 1)], 4
    while size < tiles:
        stages.append((size,))
        size *= 2
    return stages


def halve(chunks, tile, bit):
    mine = (tile // bit) % 2
    keeps, sends = [], []
    for keep, got in chunks:
        shape = (keep.shape[0] // 2, 2) + keep.shape[1:]
        keep, got = keep.reshape(shape), got.reshape(shape)
        for side, out in ((1 - mine, sends), (mine, keeps)):
            out.append(
                lax.dynamic_index_in_dim(keep, side, 1, False)
                + lax.dynamic_index_in_dim(got, side, 1, False)
            )
    return [(keep, exchange(send, "tile", bit)) for keep, send in zip(keeps, sends)]


ANY = pl.BlockSpec(memory_space=pl.ANY)
VMEM = pl.BlockSpec(memory_space=pltpu.MemorySpace.VMEM)
PARAMS = pltpu.CompilerParams(vmem_limit_bytes=16 * 1024 * 1024)
SMEM = pl.BlockSpec(memory_space=pltpu.MemorySpace.SMEM)


def local(
    northward_speed_field,
    level_depth_extent,
    potential_warmth_anomaly,
    ocean_region_label,
    zone_for_parallel,
):
    members_here, layers, columns, lats = northward_speed_field.shape
    tiles = lax.axis_size("tile")
    groups = lax.axis_size("member")
    members = members_here * groups
    per_block = LANES // SUB // tiles
    half = lats // LANES // 2
    count = groups // 2
    slots = members_here + 1
    assert lats == groups * tiles * SUB and groups * HEAT_LANES <= LANES
    assert half >= 1 and half * per_block == count and lats == 2 * half * LANES
    rows = members_here * layers * columns
    sizes = dict(
        half=half, members_here=members_here, layers=layers, columns=columns,
        groups=groups, tiles=tiles,
    )
    blocked = [
        pltpu.with_memory_space_constraint(
            x.reshape(rows // columns, columns, 2 * half, LANES)
            .transpose(0, 2, 1, 3)
            .reshape(2 * half * rows, LANES),
            pltpu.MemorySpace.HBM,
        )
        for x in (northward_speed_field, level_depth_extent, potential_warmth_anomaly)
    ]
    labels = pltpu.with_memory_space_constraint(ocean_region_label, pltpu.MemorySpace.HBM)
    early = pltpu.VMEM((tiles // 2, count * slots, SUB, LANES), jnp.float32)
    late = pltpu.VMEM((tiles // 2, count * slots + 1, SUB, LANES), jnp.float32)
    keep0, send0, heat, data, mask, spacing = pl.pallas_call(
        functools.partial(first_kernel, **sizes),
        out_shape=(
            early,
            early,
            pltpu.VMEM((LANES, LANES), jnp.float32),
            pltpu.VMEM((3, 2 * half * rows, LANES), jnp.float32),
            pltpu.VMEM((2 * half, BASINS, columns, SUB, LANES), jnp.float32),
            pltpu.VMEM((1, lats), jnp.float32),
        ),
        in_specs=[ANY] * 4,
        out_specs=(VMEM,) * 6,
        scratch_shapes=[
            pltpu.VMEM((columns, lats), jnp.int32),
            pltpu.SemaphoreType.DMA((3,)),
            pltpu.SemaphoreType.DMA(()),
        ],
        compiler_params=PARAMS,
        name="first",
    )(*blocked, labels)
    got0 = exchange(send0, "tile", 1)
    keep1, send1 = pl.pallas_call(
        functools.partial(second_kernel, **sizes),
        out_shape=(late, late),
        in_specs=[VMEM] * 4,
        out_specs=(VMEM, VMEM),
        compiler_params=PARAMS,
        name="second",
    )(data, mask, spacing, heat)
    got1 = exchange(send1, "tile", 1)
    bands = pl.pallas_call(
        functools.partial(bands_kernel, members=members, groups=groups, tiles=tiles),
        out_shape=pltpu.VMEM((groups, NBANDS * members, members * SUB), jnp.bfloat16),
        in_specs=[SMEM, ANY],
        out_specs=VMEM,
        compiler_params=PARAMS,
        name="bands",
    )(zone_for_parallel, got0)
    tile = lax.axis_index("tile")
    chunks = [(keep0, got0), (keep1, got1)]
    bit = 2
    while bit < tiles:
        chunks = halve(chunks, tile, bit)
        bit *= 2
    owned = jnp.concatenate([(keep + got)[0] for keep, got in chunks], 0)
    parts = [owned] + [exchange(owned, "member", r) for r in range(1, groups)]
    known = dict(members_here=members_here, layers=layers, groups=groups)
    share = pl.pallas_call(
        functools.partial(share_kernel, **known),
        out_shape=pltpu.VMEM((members, NBANDS * members), jnp.float32),
        in_specs=[VMEM] * (1 + groups),
        out_specs=VMEM,
        scratch_shapes=[pltpu.VMEM((groups, groups * slots, SUB, LANES), jnp.float32)],
        compiler_params=PARAMS,
        name="share",
    )(bands, *parts)
    psi, heat = pl.pallas_call(
        functools.partial(means_kernel, **known),
        out_shape=(
            jax.ShapeDtypeStruct((BASINS, SUB, layers), jnp.float32),
            jax.ShapeDtypeStruct((SUB, BASINS), jnp.float32),
        ),
        in_specs=[VMEM] * groups,
        out_specs=(VMEM, VMEM),
        compiler_params=PARAMS,
        name="means",
    )(*parts)
    norm = float((members - 1) * BASINS * layers * (lats // NBANDS))
    stages = sum_stages(tiles)
    for stage in stages[:-1]:
        gots = [exchange(share, "tile", r) for r in stage]
        for got in gots:
            share = share + got
    gots = [exchange(share, "tile", r) for r in stages[-1]]
    covariance = pl.pallas_call(
        functools.partial(unpack_kernel, members=members, scale=1.0 / norm),
        out_shape=jax.ShapeDtypeStruct((NBANDS, members, members), jnp.float32),
        in_specs=[VMEM] * (1 + len(gots)),
        out_specs=VMEM,
        compiler_params=PARAMS,
        name="unpack",
    )(share, *gots)
    return (jnp.transpose(psi, (0, 2, 1)), jnp.transpose(heat, (1, 0)), covariance)


def solution(mesh):
    in_specs = (
        P("member", None, "tile", None),
        P("member", None, "tile", None),
        P("member", None, "tile", None),
        P("tile", None),
        P(),
    )
    out_specs = (P(None, None, ("member", "tile")), P(None, ("member", "tile")), P())
    return jax.shard_map(local, mesh=mesh, in_specs=in_specs, out_specs=out_specs, check_vma=False)
```
